32 devices in a mesh: shot: 2 (over x), gz: 16 (over z, y, core).
Axes of the slice: x: 2, y: 2, z: 4, core: 2. Of those that a mesh axis runs over, the one named last changes fastest.
Arguments:
- source_now: float32 [256, 128, 128], P(('shot', 'gz')), parts along dimension 0, may hold values from -6 to 6
- source_before: float32 [256, 128, 128], P(('shot', 'gz')), parts along dimension 0, may hold values from -6 to 6
- receiver_now: float32 [256, 128, 128], P(('shot', 'gz')), parts along dimension 0, may hold values from -6 to 6
- receiver_before: float32 [256, 128, 128], P(('shot', 'gz')), parts along dimension 0, may hold values from -6 to 6
- speed_term: float32 [128, 128, 128], P('gz'), may hold values from 0.03 to 0.18
- saved_faces: float32 [24, 8, 128, 128], P('shot', None, 'gz'), parts along dimension 0, may hold values from -6 to 6
- face_steps: int32 [12], replicated, may hold values from 0 to 11, each once
- traces: bfloat16 [24, 128, 128], P('shot'), parts along dimension 0, may hold values from -6 to 6
- lag_offsets: int32 [8], replicated, may hold values from -8 to 8, as said below
- snap_phase: int32 [2], replicated, may hold values from 0 to 5
Outputs:
- image_out: bfloat16 [16, 128, 128, 128], P('shot', None, 'gz'), parts along dimension 0
- source_final: float32 [256, 128, 128], P(('shot', 'gz')), parts along dimension 0
- receiver_final: float32 [256, 128, 128], P(('shot', 'gz')), parts along dimension 0
The draws below stay inside these ranges and needn't reach their ends.
There are 2 independent parts, one for each index of `shot`. The reference program is written for one: setup_inputs(seed, part) draws one part's arguments, and reference() takes and returns one part's arrays. A program takes and returns all parts, laid end to end along the dimension named above; an argument that names none is the same for every part. Nothing has to cross between parts.
Inputs may be any that keep to these rules, and one draw needn't show every extreme that they name: `face_steps`: each of the 12 saved slots belongs to exactly one step. `lag_offsets`: the 8 offsets are different, and both ends of the range occur.
All inputs are finite; a program needn't handle non-finite values.
Results may differ from the reference program's by a relative error of at most 0.001.
Values sent between devices are 32-bit elements; how exact they have to be, the bound alone decides.
A program may use at most 64 MiB of HBM per device.

```python
import math
import jax
import jax.numpy as jnp
from jax import lax

NY = 128
NX = 128
LAGS = 8
LMAX = 8
STEPS = 12
SNAP_EVERY = 6
SNAPS = 2
NZ = 128


def draw_lag_offsets(key, part):
    first_key = jax.random.fold_in(key, 11)
    second_key = jax.random.fold_in(key, 12)
    interior = jax.random.permutation(first_key, 2 * LMAX - 1)[:LAGS - 2].astype(jnp.int32) - (LMAX - 1)
    ends_fixed = jnp.array([-LMAX, LMAX], jnp.int32)
    combined = jnp.concatenate([ends_fixed, interior])
    shuffle = jax.random.permutation(second_key, LAGS)
    return combined[shuffle]


def steps_of(key, extent, split, low, largest):
    factor_of = 1.0
    for position, shards_of in split:
        steps = jax.random.uniform(jax.random.fold_in(jax.random.fold_in(key, 6), position), (shards_of,), jnp.float32, low / len(split), largest / len(split))
        factor_of = factor_of * jnp.repeat(jnp.exp(steps), extent[position] // shards_of).reshape((-1,) + (1,) * (len(extent) - 1 - position))
    return factor_of


def gaussian(own_key, dims, spread, reach, split=(), kind=jnp.bfloat16):
    values = jax.random.normal(own_key, dims, jnp.float32) * spread
    if len(split) > 0:
        values = steps_of(own_key, dims, split, -0.22, 0.18) * values
    return jnp.clip(values, min=-reach, max=reach).astype(kind)


def setup_inputs(seed: int = 0, part: int = 0) -> dict:
    arg_keys = jax.random.split(jax.random.key(seed), 11)
    own_keys = jax.random.split(jax.random.fold_in(arg_keys[10], part), 11)
    source_now = gaussian(own_keys[0], (NZ, NY, NX), 1.0, 6.0, ((0, 16),), jnp.float32)
    source_before = gaussian(own_keys[1], (NZ, NY, NX), 1.0, 6.0, ((0, 16),), jnp.float32)
    receiver_now = gaussian(own_keys[2], (NZ, NY, NX), 1.0, 6.0, ((0, 16),), jnp.float32)
    receiver_before = gaussian(own_keys[3], (NZ, NY, NX), 1.0, 6.0, ((0, 16),), jnp.float32)
    speed_term = jnp.clip(jnp.exp(math.log(0.18) - 1.7917595 * jax.random.uniform(arg_keys[4], (NZ, NY, NX), jnp.float32) ** steps_of(arg_keys[4], (NZ, NY, NX), ((0, 16),), -0.2, 0.2)), 0.03, 0.18)
    saved_faces = gaussian(own_keys[5], (STEPS, 8, NZ, NY), 1.0, 6.0, ((2, 16),), jnp.float32)
    face_steps = jax.random.permutation(arg_keys[6], STEPS).astype(jnp.int32)
    traces = gaussian(own_keys[7], (STEPS, NY, NX), 1.0, 6.0)
    lag_offsets = draw_lag_offsets(jax.random.fold_in(arg_keys[10], 71), part)
    snap_phase = jax.random.randint(arg_keys[9], (SNAPS,), 0, SNAP_EVERY).astype(jnp.int32)
    return {"source_now": source_now, "source_before": source_before, "receiver_now": receiver_now, "receiver_before": receiver_before, "speed_term": speed_term, "saved_faces": saved_faces, "face_steps": face_steps, "traces": traces, "lag_offsets": lag_offsets, "snap_phase": snap_phase}


stencil_weights = (-205.0 / 72.0, 8.0 / 5.0, -1.0 / 5.0, 8.0 / 315.0, -1.0 / 560.0)
damping = 0.25
smoothing = 16.0

def stencil(extended, layers):
    center = extended[:, 4:4 + layers]
    height = center.shape[2]
    breadth = center.shape[3]
    padded = jnp.pad(center, ((0, 0), (0, 0), (4, 4), (4, 4)))
    summed = 3.0 * stencil_weights[0] * center
    for offset in range(1, 5):
        weight = stencil_weights[offset]
        summed = summed + weight * (extended[:, 4 + offset:4 + offset + layers] + extended[:, 4 - offset:4 - offset + layers])
        summed = summed + weight * (padded[:, :, 4 + offset:4 + offset + height, 4:4 + breadth] + padded[:, :, 4 - offset:4 - offset + height, 4:4 + breadth])
        summed = summed + weight * (padded[:, :, 4:4 + height, 4 + offset:4 + offset + breadth] + padded[:, :, 4:4 + height, 4 - offset:4 - offset + breadth])
    return summed

def advance(extended, center, previous, speed_term, faces_now, trace_now, top_row, layers):
    updated = 2.0 * center - previous + speed_term * stencil(extended, layers)
    left_faces = jnp.moveaxis(faces_now[:4], 0, -1)
    right_faces = jnp.moveaxis(faces_now[4:], 0, -1)
    source = updated[0].at[:, :, :4].set(left_faces).at[:, :, -4:].set(right_faces)
    top_mask = lax.broadcasted_iota(jnp.int32, (layers, 1, 1), 0) == top_row
    receiver = updated[1] + jnp.where(top_mask, trace_now[None], 0.0)
    return jnp.stack([source, receiver])

def lag_images(snapshot, lag_offsets):
    source = snapshot[0]
    receiver = snapshot[1]
    margin = ((0, 0), (0, 0), (LMAX, LMAX))
    source_pad = jnp.pad(source, margin)
    receiver_pad = jnp.pad(receiver, margin)
    breadth = source.shape[2]
    images = []
    for lag_index in range(LAGS):
        lag_now = lag_offsets[lag_index]
        shifted_source = lax.dynamic_slice_in_dim(source_pad, LMAX - lag_now, breadth, 2)
        shifted_receiver = lax.dynamic_slice_in_dim(receiver_pad, LMAX + lag_now, breadth, 2)
        images.append(shifted_source * shifted_receiver)
    return (jnp.stack(images), source * source)

def finish(raw_image, illumination):
    layers = illumination.shape[0]
    columns = illumination.reshape(layers, -1)
    lower = jnp.full((layers,), -smoothing, illumination.dtype).at[0].set(0.0)
    upper = jnp.full((layers,), -smoothing, illumination.dtype).at[-1].set(0.0)
    middle = jnp.full((layers,), 1.0 + 2.0 * smoothing, illumination.dtype)
    smooth = lax.linalg.tridiagonal_solve(lower, middle, upper, columns).reshape(illumination.shape)
    return (raw_image / (smooth + damping)).astype(jnp.bfloat16)

def reference(source_now, source_before, receiver_now, receiver_before, speed_term, saved_faces, face_steps, traces, lag_offsets, snap_phase):
    current = jnp.stack([source_now, receiver_now])
    previous = jnp.stack([source_before, receiver_before])
    layers = source_now.shape[0]
    zero_rows = jnp.zeros((2, 4) + source_now.shape[1:], source_now.dtype)
    raw_parts = []
    light_parts = []
    for window in range(SNAPS):
        snapshot = jnp.zeros_like(current)
        for local_index in range(SNAP_EVERY):
            step_index = window * SNAP_EVERY + local_index
            extended = jnp.concatenate([zero_rows, current, zero_rows], axis=1)
            updated = advance(extended, current, previous, speed_term, saved_faces[face_steps[step_index]], traces[step_index].astype(jnp.float32), 0, layers)
            snapshot = jnp.where(local_index == snap_phase[window], updated, snapshot)
            previous = current
            current = updated
        raw_now, light_now = lag_images(snapshot, lag_offsets)
        raw_parts.append(raw_now)
        light_parts.append(light_now)
    raw_image = raw_parts[0]
    illumination = light_parts[0]
    for window in range(1, SNAPS):
        raw_image = raw_image + raw_parts[window]
        illumination = illumination + light_parts[window]
    return (finish(raw_image, illumination), current[0], current[1])
```

```python
import functools

import jax
import jax.numpy as jnp
import numpy as np
from jax import lax
from jax.experimental import pallas as pl
from jax.experimental.pallas import tpu as pltpu
from jax.sharding import PartitionSpec as P

SNAP_EVERY = 6
SNAPS = 2
STEPS = SNAPS * SNAP_EVERY
HALO = 4
ROWS = 8
CHUNK = 4
GROUP = 4
PIECES = 4
EPOCH = 4
EPOCHS = STEPS // EPOCH

stencil_weights = (-205.0 / 72.0, 8.0 / 5.0, -1.0 / 5.0, 8.0 / 315.0, -1.0 / 560.0)
damping = 0.25
smoothing = 16.0
MESH = pl.DeviceIdType.MESH


def lateral_weights(breadth):
    apart = np.abs(np.arange(breadth)[:, None] - np.arange(breadth)[None, :])
    band = np.zeros((breadth, breadth), np.float64)
    band[apart == 0] = 3.0 * stencil_weights[0]
    for offset in range(1, 5):
        band[apart == offset] = stencil_weights[offset]
    band = jnp.asarray(band, jnp.float32)
    high = band.astype(jnp.bfloat16)
    low = (band - high.astype(jnp.float32)).astype(jnp.bfloat16)
    return jnp.concatenate([high, high], axis=0), low


def wave_kernel(
    count,
    strip,
    phase_ref,
    order_ref,
    src_now,
    src_old,
    rec_now,
    rec_old,
    speed,
    faces,
    traces,
    weights_a,
    weights_b,
    strips_out,
    src_out,
    rec_out,
    field,
    factor,
    packed,
    edges,
    halo,
    snaps,
    load_send,
    load_recv,
    load_own,
    edge_send,
    edge_recv,
    z_send,
    z_recv,
    row_send,
    row_recv,
    strip_send,
    strip_recv,
    strip_own,
    back_send,
    back_recv,
    back_own,
):
    me = lax.axis_index("gz")
    outer = count // GROUP
    a = me // GROUP
    b = me % GROUP
    kind = b // 2
    c = b % 2
    thin = src_now.shape[0]
    layers = thin * GROUP
    height = src_now.shape[1] // 2
    breadth = src_now.shape[2]
    inner = pl.ds(ROWS, height)
    now_of = (src_now, rec_now)
    old_of = (src_old, rec_old)
    outs = (src_out, rec_out)

    def load_refs(index, target, sender):
        rows = pl.ds(target % 2 * height, height)
        planes = pl.ds(HALO + sender * thin, thin)
        source = (speed, now_of[target // 2], old_of[target // 2])[index]
        landed = (
            factor.at[pl.ds(sender * thin, thin)],
            field.at[0, planes, inner],
            field.at[1, planes, inner],
        )[index]
        return source.at[:, rows, :], landed

    def load_remote(index, target, sender):
        source, landed = load_refs(index, target, sender)
        return pltpu.make_async_remote_copy(
            src_ref=source,
            dst_ref=landed,
            send_sem=load_send.at[index, target],
            recv_sem=load_recv.at[index, sender],
            device_id={"gz": a * GROUP + target},
            device_id_type=MESH,
        )

    def load_local(index, target):
        source, landed = load_refs(index, target, target)
        return pltpu.make_async_copy(source, landed, load_own.at[index])

    for index in range(3):
        for target in range(GROUP):

            @pl.when(b != target)
            def _():
                load_remote(index, target, b).start()

    for index in range(3):
        for target in range(GROUP):

            @pl.when(b == target)
            def _():
                load_local(index, target).start()

    def wait_load(index):
        for sender in range(GROUP):

            @pl.when(b == sender)
            def _():
                load_local(index, sender).wait()

            @pl.when(b != sender)
            def _():
                load_remote(index, sender, sender).wait_recv()

    lane = lax.broadcasted_iota(jnp.int32, (1, 1, breadth), 2)
    across = 8 * EPOCH
    groups = breadth // across
    tall = height // groups
    for z in range(thin):
        parts = [
            pltpu.roll(faces[order_ref[step], :, z, :], 4, 0) for step in range(STEPS)
        ]
        parts.append(jnp.zeros((breadth - 8 * STEPS, 2 * height), jnp.float32))
        turned = jnp.concatenate(parts, axis=0).T
        for epoch in range(EPOCHS):
            for half in range(2):
                block = None
                for part in range(groups):
                    first = half * height + part * tall
                    moved = turned[first : first + tall]
                    turn = (across * (part - epoch)) % breadth
                    if turn:
                        moved = pltpu.roll(moved, turn, 1)
                    if block is None:
                        block = moved
                    else:
                        block = jnp.where(lane[0] >= across * part, moved, block)
                packed[epoch, half, z] = block

    def edge_remote(epoch, target, sender):
        return pltpu.make_async_remote_copy(
            src_ref=packed.at[epoch, target],
            dst_ref=edges.at[epoch, pl.ds(sender * thin, thin)],
            send_sem=edge_send.at[epoch, target],
            recv_sem=edge_recv.at[epoch, sender],
            device_id={"gz": a * GROUP + target},
            device_id_type=MESH,
        )

    for epoch in range(EPOCHS):
        for target in range(2):

            @pl.when(b != target)
            def _():
                edge_remote(epoch, target, b).start()

            @pl.when(b == target)
            def _():
                edges[epoch, pl.ds(target * thin, thin)] = packed[epoch, target]

    def wait_edge(epoch):
        for sender in range(GROUP):

            @pl.when(jnp.logical_and(kind == 0, b != sender))
            def _():
                edge_remote(epoch, 0, sender).wait_recv()

    for slot in range(2):
        for first in (0, HALO + layers):
            field[slot, pl.ds(first, HALO), inner] = jnp.zeros(
                (HALO, height, breadth), jnp.float32
            )

        @pl.when(c == 0)
        def _():
            field[slot, pl.ds(HALO, layers), pl.ds(0, ROWS)] = jnp.zeros(
                (layers, ROWS, breadth), jnp.float32
            )

        @pl.when(c == 1)
        def _():
            field[slot, pl.ds(HALO, layers), pl.ds(ROWS + height, ROWS)] = jnp.zeros(
                (layers, ROWS, breadth), jnp.float32
            )

        @pl.when(a == 0)
        def _():
            halo[0, slot] = jnp.zeros((HALO, height, breadth), jnp.float32)

        @pl.when(a == outer - 1)
        def _():
            halo[1, slot] = jnp.zeros((HALO, height, breadth), jnp.float32)

    snaps[...] = jnp.zeros(snaps.shape, jnp.float32)

    span = height // PIECES
    present = (a > 0, a < outer - 1)

    def z_copy(side, piece, slot):
        return pltpu.make_async_remote_copy(
            src_ref=field.at[
                slot,
                pl.ds((HALO, layers)[side], HALO),
                pl.ds(ROWS + piece * span, span),
            ],
            dst_ref=halo.at[1 - side, slot, :, pl.ds(piece * span, span)],
            send_sem=z_send.at[side, slot, piece],
            recv_sem=z_recv.at[1 - side, slot, piece],
            device_id={"gz": (me - GROUP, me + GROUP)[side]},
            device_id_type=MESH,
        )

    def send_z(piece, slot, also=None):
        for side in range(2):
            allowed = present[side]
            if also is not None:
                allowed = jnp.logical_and(allowed, also)

            @pl.when(allowed)
            def _():
                z_copy(side, piece, slot).start()

    def wait_z(piece, slot):
        for side in range(2):

            @pl.when(present[side])
            def _():
                z_copy(1 - side, piece, slot).wait_recv()

    def sent_z(slot):
        for side in range(2):

            @pl.when(present[side])
            def _():
                for piece in range(PIECES):
                    z_copy(side, piece, slot).wait_send()

    body = pl.ds(HALO, layers)

    def row_copy(way, slot):
        first, landed = (
            (ROWS + height - HALO, ROWS - HALO),
            (ROWS, ROWS + height),
        )[way]
        return pltpu.make_async_remote_copy(
            src_ref=field.at[slot, body, pl.ds(first, HALO)],
            dst_ref=field.at[slot, body, pl.ds(landed, HALO)],
            send_sem=row_send.at[slot],
            recv_sem=row_recv.at[slot],
            device_id={"gz": me + 1 - 2 * c},
            device_id_type=MESH,
        )

    def each_way(do, also=None):
        for way in range(2):
            allowed = c == way
            if also is not None:
                allowed = jnp.logical_and(allowed, also)

            @pl.when(allowed)
            def _():
                do(way)

    def send_row(slot, also=None):
        each_way(lambda way: row_copy(way, slot).start(), also)

    def wait_row(slot):
        each_way(lambda way: row_copy(1 - way, slot).wait_recv())

    def sent_row(slot):
        each_way(lambda way: row_copy(way, slot).wait_send())

    outside = ((lane < 4) | (lane >= breadth - 4)) & (kind == 0)
    lit = jnp.logical_and(a == 0, kind == 1)

    def partial(step, now, later, base, top):
        planes = pl.ds(HALO + base, CHUNK)
        center = field[now, planes, inner, :]
        flat = center.reshape(CHUNK * height, breadth)
        high = flat.astype(jnp.bfloat16)
        low = (flat - high.astype(jnp.float32)).astype(jnp.bfloat16)
        lateral = jnp.dot(
            jnp.concatenate([high, low], axis=1),
            weights_a[...],
            preferred_element_type=jnp.float32,
        ) + jnp.dot(high, weights_b[...], preferred_element_type=jnp.float32)
        summed = lateral.reshape(CHUNK, height, breadth)
        for offset in range(1, 5):
            summed = summed + stencil_weights[offset] * (
                (
                    field[now, pl.ds(HALO + base + offset, CHUNK), inner, :]
                    + field[now, pl.ds(HALO + base - offset, CHUNK), inner, :]
                )
                + (
                    field[now, planes, pl.ds(ROWS + offset, height), :]
                    + field[now, planes, pl.ds(ROWS - offset, height), :]
                )
            )
        previous = field[later, planes, inner, :]
        updated = 2.0 * center - previous + factor[pl.ds(base, CHUNK)] * summed
        edge = edges[step // EPOCH, pl.ds(base, CHUNK)].reshape(CHUNK * tall, breadth)
        placed = jnp.concatenate(
            [
                pltpu.roll(
                    edge,
                    lax.rem(
                        3 * breadth - 4 - across * part - 8 * (step % EPOCH), breadth
                    ),
                    1,
                ).reshape(CHUNK, tall, breadth)
                for part in range(groups)
            ],
            axis=1,
        )
        updated = jnp.where(outside, placed, updated)
        if top:
            trace = traces[step, pl.ds(pl.multiple_of(c * height, height), height)]
            trace = jnp.where(lit, trace.astype(jnp.float32), 0.0)
            updated = jnp.concatenate([updated[:1] + trace[None], updated[1:]], axis=0)
        return updated

    def keep(window, take, base, rows, value):
        held = snaps[window, pl.ds(base, value.shape[0]), rows]
        snaps[window, pl.ds(base, value.shape[0]), rows] = jnp.where(take, value, held)

    def complete(window, take, now, later, piece):
        rows = pl.ds(piece * span, span)
        wide = pl.ds(ROWS + piece * span, span)
        for side in range(2):
            base = (0, layers - HALO)[side]
            held = [halo[side, now, near, rows] for near in range(HALO)]
            added = []
            for near in range(HALO):
                total = None
                reach = HALO - near if side == 0 else near + 1
                for k in range(reach):
                    offset = HALO - k
                    index = near + k if side == 0 else near - k
                    term = stencil_weights[offset] * held[index]
                    total = term if total is None else total + term
                added.append(total[None])
            added = jnp.concatenate(added, axis=0)
            planes = pl.ds(HALO + base, HALO)
            value = (
                field[later, planes, wide] + factor[pl.ds(base, HALO), rows] * added
            )
            field[later, planes, wide] = value
            keep(window, take, base, rows, value)

    whole = pl.ds(0, height)

    def whole_step(window, local):
        step = window * SNAP_EVERY + local
        now = lax.rem(step, 2)
        later = 1 - now
        more = step < STEPS - 1
        take = phase_ref[window] == local

        @pl.when(lax.rem(step, EPOCH) == 0)
        def _():
            wait_edge(step // EPOCH)

        wait_row(now)
        for base, top in ((0, True), (layers - HALO, False)):
            field[later, pl.ds(HALO + base, CHUNK), inner] = partial(
                step, now, later, base, top
            )
        for piece in range(PIECES):
            wait_z(piece, now)
            complete(window, take, now, later, piece)
            send_z(piece, later, more)

        def middle(chunk, carried):
            base = chunk * CHUNK
            value = partial(step, now, later, base, False)
            field[later, pl.ds(HALO + base, CHUNK), inner] = value
            keep(window, take, base, whole, value)
            return carried

        lax.fori_loop(1, layers // CHUNK - 1, middle, 0)
        send_row(later, more)
        sent_z(now)
        sent_row(now)

    half = count // 2

    def strip_refs(window, index):
        first = pl.multiple_of(index * strip // ROWS * ROWS, ROWS)
        return (
            snaps.at[window, :, pl.ds(first, ROWS), :],
            strips_out.at[window, kind, pl.ds(a * layers, layers)],
        )

    def strip_remote(window, index, sender, sort):
        source = snaps.at[
            window, :, pl.ds(pl.multiple_of(index * strip // ROWS * ROWS, ROWS), ROWS), :
        ]
        return pltpu.make_async_remote_copy(
            src_ref=source,
            dst_ref=strips_out.at[window, sort, pl.ds(sender * layers, layers)],
            send_sem=strip_send.at[window, index],
            recv_sem=strip_recv.at[window, sort, sender],
            device_id={"gz": c * half + index},
            device_id_type=MESH,
        )

    def strip_local(window, index):
        source, landed = strip_refs(window, index)
        return pltpu.make_async_copy(source, landed, strip_own.at[window])

    def start_strip(window, turn):
        index = (turn + GROUP * a + 2 * kind) % half
        target = c * half + index

        @pl.when(jnp.logical_and(target != me, turn < half))
        def _():
            strip_remote(window, index, a, kind).start()

        @pl.when(jnp.logical_and(target == me, turn < half))
        def _():
            strip_local(window, index).start()

    def finish_strips(window):
        def sent(index, carried):
            target = c * half + index

            @pl.when(target != me)
            def _():
                strip_remote(window, index, a, kind).wait_send()

            @pl.when(target == me)
            def _():
                strip_local(window, index).wait()

            return carried

        lax.fori_loop(0, half, sent, 0)
        for sort in range(2):
            for sender in range(outer):

                @pl.when(sender * GROUP + 2 * sort + me // half != me)
                def _():
                    strip_remote(window, 0, sender, sort).wait_recv()

    wait_load(1)
    for piece in range(PIECES):
        send_z(piece, 0)
    send_row(0)
    wait_load(0)

    def mask(layer, carried):
        factor[layer] = jnp.where(outside[0], 0.0, factor[layer])
        return carried

    lax.fori_loop(0, layers, mask, 0)
    wait_load(2)
    for index in range(3):
        for target in range(GROUP):

            @pl.when(b != target)
            def _():
                load_remote(index, target, b).wait_send()

    share = (half + SNAP_EVERY - 1) // SNAP_EVERY
    for window in range(SNAPS):

        def both(local, carried):
            whole_step(window, local)
            if window > 0:
                for part in range(share):
                    start_strip(window - 1, local * share + part)
            return carried

        lax.fori_loop(0, SNAP_EVERY, both, 0)
    lax.fori_loop(0, half, lambda turn, carried: (start_strip(SNAPS - 1, turn), carried)[1], 0)

    last = STEPS % 2

    def back_refs(sort, target):
        return (
            field.at[last, pl.ds(HALO + target * thin, thin), inner],
            outs[sort].at[:, pl.ds(pl.multiple_of(c * height, height), height), :],
        )

    def back_remote(sort, target):
        source, landed = back_refs(sort, target)
        return pltpu.make_async_remote_copy(
            src_ref=source,
            dst_ref=landed,
            send_sem=back_send.at[target],
            recv_sem=back_recv.at[sort, c],
            device_id={"gz": a * GROUP + target},
            device_id_type=MESH,
        )

    def back_arrival(sort, side):
        return pltpu.make_async_remote_copy(
            src_ref=field.at[last, pl.ds(HALO, thin), inner],
            dst_ref=outs[sort].at[:, pl.ds(side * height, height), :],
            send_sem=back_send.at[0],
            recv_sem=back_recv.at[sort, side],
            device_id={"gz": a * GROUP + 2 * sort + side},
            device_id_type=MESH,
        )

    def back_local(sort, target):
        source, landed = back_refs(sort, target)
        return pltpu.make_async_copy(source, landed, back_own.at[0])

    def each_back(remote, own):
        for sort in range(2):
            for target in range(GROUP):

                @pl.when(jnp.logical_and(kind == sort, b != target))
                def _():
                    remote(sort, target)

                if target // 2 == sort:

                    @pl.when(b == target)
                    def _():
                        own(sort, target)

    each_back(
        lambda sort, target: back_remote(sort, target).start(),
        lambda sort, target: back_local(sort, target).start(),
    )
    for epoch in range(EPOCHS):
        for target in range(2):

            @pl.when(b != target)
            def _():
                edge_remote(epoch, target, b).wait_send()

    each_back(
        lambda sort, target: back_remote(sort, target).wait_send(),
        lambda sort, target: back_local(sort, target).wait(),
    )
    for sort in range(2):
        for side in range(2):

            @pl.when(b != 2 * sort + side)
            def _():
                back_arrival(sort, side).wait_recv()

    for window in range(SNAPS):
        finish_strips(window)


def image_kernel(lag_ref, pivot_ref, strips, image, inverse):
    depth = strips.shape[2]
    breadth = strips.shape[4]
    lags = image.shape[0]
    unit = strips.shape[3:]

    def down(z, carried):
        first = strips[0, 0, z]
        second = strips[1, 0, z]
        value = (first * first + second * second + smoothing * carried) * pivot_ref[z]
        inverse[z] = value
        return value

    lax.fori_loop(0, depth, down, jnp.zeros(unit, jnp.float32), unroll=8)

    def up(turn, carried):
        z = depth - 1 - turn
        value = inverse[z] + (smoothing * pivot_ref[z]) * carried
        inverse[z] = 1.0 / (value + damping)
        return value

    lax.fori_loop(0, depth, up, jnp.zeros(unit, jnp.float32), unroll=8)

    lane = lax.broadcasted_iota(jnp.int32, unit, 1)
    some = 32
    for index in range(lags):
        lag = lag_ref[index]
        reach = jnp.abs(lag)
        inside = (lane >= reach) & (lane < breadth - reach)
        back = lax.rem(2 * breadth - 2 * lag, breadth)
        forth = lax.rem(breadth + lag, breadth)

        def layers(block, carried):
            z = pl.ds(block * some, some)
            raw = strips[0, 0, z] * pltpu.roll(strips[0, 1, z], back, 2)
            raw = raw + strips[1, 0, z] * pltpu.roll(strips[1, 1, z], back, 2)
            raw = jnp.where(inside[None], pltpu.roll(raw, forth, 2), 0.0)
            image[index, z] = (raw * inverse[z]).astype(jnp.bfloat16)
            return carried

        lax.fori_loop(0, depth // some, layers, 0)


def local(
    count,
    source_now,
    source_before,
    receiver_now,
    receiver_before,
    speed_term,
    saved_faces,
    face_steps,
    traces,
    lag_offsets,
    snap_phase,
):
    thin, wide, breadth = source_now.shape
    layers = thin * GROUP
    outer = count // GROUP
    half = count // 2
    depth = thin * count
    height = wide // 2
    strip = wide // count
    tall = height * 8 * EPOCH // breadth
    me = lax.axis_index("gz")
    weights_a, weights_b = lateral_weights(breadth)

    any_space = pl.BlockSpec(memory_space=pl.ANY)
    vmem = pl.BlockSpec(memory_space=pltpu.VMEM)
    smem = pl.BlockSpec(memory_space=pltpu.SMEM)
    dma = pltpu.SemaphoreType.DMA
    flat = jax.ShapeDtypeStruct(source_now.shape, jnp.float32)
    strips, source_final, receiver_final = pl.pallas_call(
        functools.partial(wave_kernel, count, strip),
        out_shape=(
            jax.ShapeDtypeStruct((SNAPS, 2, depth, ROWS, breadth), jnp.float32),
            flat,
            flat,
        ),
        in_specs=[smem] * 2 + [any_space] * 5 + [vmem] * 4,
        out_specs=(any_space, any_space, any_space),
        scratch_shapes=[
            pltpu.VMEM((2, layers + 2 * HALO, height + 2 * ROWS, breadth), jnp.float32),
            pltpu.VMEM((layers, height, breadth), jnp.float32),
            pltpu.VMEM((EPOCHS, 2, thin, tall, breadth), jnp.float32),
            pltpu.VMEM((EPOCHS, layers, tall, breadth), jnp.float32),
            pltpu.VMEM((2, 2, HALO, height, breadth), jnp.float32),
            pltpu.VMEM((SNAPS, layers, height, breadth), jnp.float32),
            dma((3, GROUP)),
            dma((3, GROUP)),
            dma((3,)),
            dma((EPOCHS, 2)),
            dma((EPOCHS, GROUP)),
            dma((2, 2, PIECES)),
            dma((2, 2, PIECES)),
            dma((2,)),
            dma((2,)),
            dma((SNAPS, half)),
            dma((SNAPS, 2, outer)),
            dma((SNAPS,)),
            dma((GROUP,)),
            dma((2, 2)),
            dma((1,)),
        ],
        compiler_params=pltpu.CompilerParams(
            has_side_effects=True, vmem_limit_bytes=40 * 1024 * 1024
        ),
        name="waves",
    )(
        snap_phase,
        face_steps,
        source_now,
        source_before,
        receiver_now,
        receiver_before,
        speed_term,
        saved_faces,
        traces,
        weights_a,
        weights_b,
    )

    if strip < ROWS:
        strips = lax.dynamic_slice_in_dim(strips, (me * strip) % ROWS, strip, 3)
    pivots = []
    pivot = 0.0
    for _ in range(depth):
        pivot = 1.0 / (1.0 + 2.0 * smoothing - smoothing * smoothing * pivot)
        pivots.append(pivot)
    image = pl.pallas_call(
        image_kernel,
        out_shape=jax.ShapeDtypeStruct(
            (lag_offsets.shape[0], depth, strip, breadth), jnp.bfloat16
        ),
        in_specs=[smem, smem, vmem],
        out_specs=vmem,
        scratch_shapes=[pltpu.VMEM((depth, strip, breadth), jnp.float32)],
        compiler_params=pltpu.CompilerParams(vmem_limit_bytes=48 * 1024 * 1024),
        name="images",
    )(lag_offsets, jnp.asarray(np.array(pivots, np.float32)), strips)
    return image, source_final, receiver_final


def solution(mesh):
    return jax.shard_map(
        functools.partial(local, mesh.shape["gz"]),
        mesh=mesh,
        in_specs=(
            P(("shot", "gz"), None, None),
            P(("shot", "gz"), None, None),
            P(("shot", "gz"), None, None),
            P(("shot", "gz"), None, None),
            P("gz", None, None),
            P("shot", None, "gz", None),
            P(),
            P("shot", None, None),
            P(),
            P(),
        ),
        out_specs=(
            P("shot", None, "gz", None),
            P(("shot", "gz"), None, None),
            P(("shot", "gz"), None, None),
        ),
        check_vma=False,
    )
```

```python
import functools

import jax
import jax.numpy as jnp
import numpy as np
from jax import lax
from jax.experimental import pallas as pl
from jax.experimental.pallas import tpu as pltpu
from jax.sharding import PartitionSpec as P

SNAP_EVERY = 6
SNAPS = 2
STEPS = SNAPS * SNAP_EVERY
HALO = 4
ROWS = 8
CHUNK = 4
GROUP = 4
PIECES = 4
EPOCH = 4
VMEM_BYTES = 60 * 1024 * 1024
EPOCHS = STEPS // EPOCH

stencil_weights = (-205.0 / 72.0, 8.0 / 5.0, -1.0 / 5.0, 8.0 / 315.0, -1.0 / 560.0)
damping = 0.25
smoothing = 16.0
MESH = pl.DeviceIdType.MESH


def lateral_weights(breadth):
    apart = jnp.abs(
        lax.broadcasted_iota(jnp.int32, (breadth, breadth), 0)
        - lax.broadcasted_iota(jnp.int32, (breadth, breadth), 1)
    )
    band = jnp.where(apart == 0, 3.0 * stencil_weights[0], 0.0)
    for offset in range(1, 5):
        band = jnp.where(apart == offset, stencil_weights[offset], band)
    high = band.astype(jnp.bfloat16)
    low = (band - high.astype(jnp.float32)).astype(jnp.bfloat16)
    return high, low


def wave_kernel(
    count,
    shots,
    strip,
    lag_ref,
    phase_hbm,
    order_hbm,
    src_now,
    src_old,
    rec_now,
    rec_old,
    speed,
    faces_hbm,
    traces_hbm,
    raw_out,
    light_out,
    src_out,
    rec_out,
    phase_ref,
    order_ref,
    faces,
    traces,
    weights_a,
    weights_b,
    field,
    factor,
    packed,
    edges,
    halo,
    snaps,
    strips,
    raw,
    light,
    small_own,
    load_send,
    load_recv,
    load_own,
    relay_send,
    relay_recv,
    edge_send,
    edge_recv,
    z_send,
    z_recv,
    row_send,
    row_recv,
    strip_send,
    strip_recv,
    strip_own,
    back_send,
    back_recv,
    back_own,
    out_own,
):
    me = lax.axis_index("gz")
    outer = count // GROUP
    a = me // GROUP
    b = me % GROUP
    kind = b // 2
    c = b % 2
    thin = src_now.shape[0]
    layers = thin * GROUP
    height = src_now.shape[1] // 2
    breadth = src_now.shape[2]
    inner = pl.ds(ROWS, height)
    now_of = (src_now, rec_now)
    old_of = (src_old, rec_old)
    outs = (src_out, rec_out)

    def load_refs(index, target, sender):
        rows = pl.ds(target % 2 * height, height)
        planes = pl.ds(HALO + sender * thin, thin)
        source = (speed, now_of[target // 2], old_of[target // 2])[index]
        landed = (
            factor.at[pl.ds(sender * thin, thin)],
            field.at[0, planes, inner],
            field.at[1, planes, inner],
        )[index]
        return source.at[:, rows, :], landed

    def load_remote(index, target, sender):
        source, landed = load_refs(index, target, sender)
        return pltpu.make_async_remote_copy(
            src_ref=source,
            dst_ref=landed,
            send_sem=load_send.at[index, target],
            recv_sem=load_recv.at[index, sender],
            device_id={"gz": a * GROUP + target},
            device_id_type=MESH,
        )

    def load_local(index, target):
        source, landed = load_refs(index, target, target)
        return pltpu.make_async_copy(source, landed, load_own.at[index])

    paired = shots % 2 == 0
    shot = lax.axis_index("shot")
    parity = shot % 2

    def direct(index, target):
        if index > 0 or not paired:
            return b != target
        near = jnp.logical_or(kind == target // 2, parity == target % 2)
        return jnp.logical_and(b != target, near)

    def relay(sender):
        view = factor.at[pl.ds(sender * thin, thin)]
        return pltpu.make_async_remote_copy(
            src_ref=view,
            dst_ref=view,
            send_sem=relay_send.at[sender % 2],
            recv_sem=relay_recv.at[sender % 2],
            device_id={"shot": shot + 1 - 2 * parity, "gz": me},
            device_id_type=MESH,
        )

    small = (
        (faces_hbm, faces),
        (order_hbm, order_ref),
        (phase_hbm, phase_ref),
        (traces_hbm, traces),
    )

    def fetch(index):
        source, landed = small[index]
        return pltpu.make_async_copy(source, landed, small_own.at[index])

    for index in range(3):
        for target in range(GROUP):

            @pl.when(direct(index, target))
            def _():
                load_remote(index, target, b).start()

    for index in range(len(small)):
        fetch(index).start()
    for index in range(3):
        for target in range(GROUP):

            @pl.when(b == target)
            def _():
                load_local(index, target).start()

    def wait_load(index):
        for sender in range(GROUP):

            @pl.when(b == sender)
            def _():
                load_local(index, sender).wait()

            if index > 0 or not paired:

                @pl.when(b != sender)
                def _():
                    load_remote(index, sender, sender).wait_recv()

            else:

                @pl.when(jnp.logical_and(b != sender, kind == sender // 2))
                def _():
                    load_remote(index, sender, sender).wait_recv()

                @pl.when(jnp.logical_and(kind != sender // 2, parity != c))
                def _():
                    relay(sender).wait_recv()

    def pass_on():
        for sender in range(GROUP):

            @pl.when(jnp.logical_and(kind != sender // 2, parity == c))
            def _():
                load_remote(0, sender, sender).wait_recv()
                relay(sender).start()

    def passed_on():
        for sender in range(GROUP):

            @pl.when(jnp.logical_and(kind != sender // 2, parity == c))
            def _():
                relay(sender).wait_send()

    high, low = lateral_weights(breadth)
    weights_a[pl.ds(0, breadth)] = high
    weights_a[pl.ds(breadth, breadth)] = high
    weights_b[...] = low
    fetch(0).wait()
    fetch(1).wait()

    lane = lax.broadcasted_iota(jnp.int32, (1, 1, breadth), 2)
    across = 8 * EPOCH
    groups = breadth // across
    tall = height // groups
    for z in range(thin):
        parts = [
            pltpu.roll(faces[order_ref[step], :, z, :], 4, 0) for step in range(STEPS)
        ]
        parts.append(jnp.zeros((breadth - 8 * STEPS, 2 * height), jnp.float32))
        turned = jnp.concatenate(parts, axis=0).T
        for epoch in range(EPOCHS):
            for half in range(2):
                block = None
                for part in range(groups):
                    first = half * height + part * tall
                    moved = turned[first : first + tall]
                    turn = (across * (part - epoch)) % breadth
                    if turn:
                        moved = pltpu.roll(moved, turn, 1)
                    if block is None:
                        block = moved
                    else:
                        block = jnp.where(lane[0] >= across * part, moved, block)
                packed[epoch, half, z] = block

    def edge_remote(epoch, target, sender):
        return pltpu.make_async_remote_copy(
            src_ref=packed.at[epoch, target],
            dst_ref=edges.at[epoch, pl.ds(sender * thin, thin)],
            send_sem=edge_send.at[epoch, target],
            recv_sem=edge_recv.at[epoch, sender],
            device_id={"gz": a * GROUP + target},
            device_id_type=MESH,
        )

    for epoch in range(EPOCHS):
        for target in range(2):

            @pl.when(b != target)
            def _():
                edge_remote(epoch, target, b).start()

            @pl.when(b == target)
            def _():
                edges[epoch, pl.ds(target * thin, thin)] = packed[epoch, target]

    def wait_edge(epoch):
        for sender in range(GROUP):

            @pl.when(jnp.logical_and(kind == 0, b != sender))
            def _():
                edge_remote(epoch, 0, sender).wait_recv()

    for slot in range(2):
        for first in (0, HALO + layers):
            field[slot, pl.ds(first, HALO), inner] = jnp.zeros(
                (HALO, height, breadth), jnp.float32
            )

        @pl.when(c == 0)
        def _():
            field[slot, pl.ds(HALO, layers), pl.ds(0, ROWS)] = jnp.zeros(
                (layers, ROWS, breadth), jnp.float32
            )

        @pl.when(c == 1)
        def _():
            field[slot, pl.ds(HALO, layers), pl.ds(ROWS + height, ROWS)] = jnp.zeros(
                (layers, ROWS, breadth), jnp.float32
            )

        @pl.when(a == 0)
        def _():
            halo[0, slot] = jnp.zeros((HALO, height, breadth), jnp.float32)

        @pl.when(a == outer - 1)
        def _():
            halo[1, slot] = jnp.zeros((HALO, height, breadth), jnp.float32)

    snaps[...] = jnp.zeros(snaps.shape, jnp.float32)

    span = height // PIECES
    present = (a > 0, a < outer - 1)

    def z_copy(side, piece, slot):
        return pltpu.make_async_remote_copy(
            src_ref=field.at[
                slot,
                pl.ds((HALO, layers)[side], HALO),
                pl.ds(ROWS + piece * span, span),
            ],
            dst_ref=halo.at[1 - side, slot, :, pl.ds(piece * span, span)],
            send_sem=z_send.at[side, slot, piece],
            recv_sem=z_recv.at[1 - side, slot, piece],
            device_id={"gz": (me - GROUP, me + GROUP)[side]},
            device_id_type=MESH,
        )

    def send_z(piece, slot, also=None):
        for side in range(2):
            allowed = present[side]
            if also is not None:
                allowed = jnp.logical_and(allowed, also)

            @pl.when(allowed)
            def _():
                z_copy(side, piece, slot).start()

    def wait_z(piece, slot):
        for side in range(2):

            @pl.when(present[side])
            def _():
                z_copy(1 - side, piece, slot).wait_recv()

    def sent_z(slot):
        for side in range(2):

            @pl.when(present[side])
            def _():
                for piece in range(PIECES):
                    z_copy(side, piece, slot).wait_send()

    body = pl.ds(HALO, layers)

    def row_copy(way, slot):
        first, landed = (
            (ROWS + height - HALO, ROWS - HALO),
            (ROWS, ROWS + height),
        )[way]
        return pltpu.make_async_remote_copy(
            src_ref=field.at[slot, body, pl.ds(first, HALO)],
            dst_ref=field.at[slot, body, pl.ds(landed, HALO)],
            send_sem=row_send.at[slot],
            recv_sem=row_recv.at[slot],
            device_id={"gz": me + 1 - 2 * c},
            device_id_type=MESH,
        )

    def each_way(do, also=None):
        for way in range(2):
            allowed = c == way
            if also is not None:
                allowed = jnp.logical_and(allowed, also)

            @pl.when(allowed)
            def _():
                do(way)

    def send_row(slot, also=None):
        each_way(lambda way: row_copy(way, slot).start(), also)

    def wait_row(slot):
        each_way(lambda way: row_copy(1 - way, slot).wait_recv())

    def sent_row(slot):
        each_way(lambda way: row_copy(way, slot).wait_send())

    outside = ((lane < 4) | (lane >= breadth - 4)) & (kind == 0)
    lit = jnp.logical_and(a == 0, kind == 1)

    def partial(step, now, later, base, top):
        planes = pl.ds(HALO + base, CHUNK)
        center = field[now, planes, inner, :]
        flat = center.reshape(CHUNK * height, breadth)
        high = flat.astype(jnp.bfloat16)
        low = (flat - high.astype(jnp.float32)).astype(jnp.bfloat16)
        lateral = jnp.dot(
            jnp.concatenate([high, low], axis=1),
            weights_a[...],
            preferred_element_type=jnp.float32,
        ) + jnp.dot(high, weights_b[...], preferred_element_type=jnp.float32)
        summed = lateral.reshape(CHUNK, height, breadth)
        for offset in range(1, 5):
            summed = summed + stencil_weights[offset] * (
                (
                    field[now, pl.ds(HALO + base + offset, CHUNK), inner, :]
                    + field[now, pl.ds(HALO + base - offset, CHUNK), inner, :]
                )
                + (
                    field[now, planes, pl.ds(ROWS + offset, height), :]
                    + field[now, planes, pl.ds(ROWS - offset, height), :]
                )
            )
        previous = field[later, planes, inner, :]
        updated = 2.0 * center - previous + factor[pl.ds(base, CHUNK)] * summed
        edge = edges[step // EPOCH, pl.ds(base, CHUNK)].reshape(CHUNK * tall, breadth)
        placed = jnp.concatenate(
            [
                pltpu.roll(
                    edge,
                    lax.rem(
                        3 * breadth - 4 - across * part - 8 * (step % EPOCH), breadth
                    ),
                    1,
                ).reshape(CHUNK, tall, breadth)
                for part in range(groups)
            ],
            axis=1,
        )
        updated = jnp.where(outside, placed, updated)
        if top:
            trace = traces[step, pl.ds(pl.multiple_of(c * height, height), height)]
            trace = jnp.where(lit, trace.astype(jnp.float32), 0.0)
            updated = jnp.concatenate([updated[:1] + trace[None], updated[1:]], axis=0)
        return updated

    def keep(window, take, base, rows, value):
        held = snaps[window, pl.ds(base, value.shape[0]), rows]
        snaps[window, pl.ds(base, value.shape[0]), rows] = jnp.where(take, value, held)

    def complete(window, take, now, later, piece):
        rows = pl.ds(piece * span, span)
        wide = pl.ds(ROWS + piece * span, span)
        for side in range(2):
            base = (0, layers - HALO)[side]
            held = [halo[side, now, near, rows] for near in range(HALO)]
            added = []
            for near in range(HALO):
                total = None
                reach = HALO - near if side == 0 else near + 1
                for k in range(reach):
                    offset = HALO - k
                    index = near + k if side == 0 else near - k
                    term = stencil_weights[offset] * held[index]
                    total = term if total is None else total + term
                added.append(total[None])
            added = jnp.concatenate(added, axis=0)
            planes = pl.ds(HALO + base, HALO)
            added = jnp.where(outside, 0.0, factor[pl.ds(base, HALO), rows] * added)
            value = field[later, planes, wide] + added
            field[later, planes, wide] = value
            keep(window, take, base, rows, value)

    whole = pl.ds(0, height)

    def whole_step(window, local):
        step = window * SNAP_EVERY + local
        now = lax.rem(step, 2)
        later = 1 - now
        more = step < STEPS - 1
        take = phase_ref[window] == local

        @pl.when(lax.rem(step, EPOCH) == 0)
        def _():
            wait_edge(step // EPOCH)

        wait_row(now)
        for base, top in ((0, True), (layers - HALO, False)):
            field[later, pl.ds(HALO + base, CHUNK), inner] = partial(
                step, now, later, base, top
            )
        for piece in range(PIECES):
            wait_z(piece, now)
            complete(window, take, now, later, piece)
            send_z(piece, later, more)

        def middle(chunk, carried):
            base = chunk * CHUNK
            value = partial(step, now, later, base, False)
            field[later, pl.ds(HALO + base, CHUNK), inner] = value
            keep(window, take, base, whole, value)
            return carried

        lax.fori_loop(1, layers // CHUNK - 1, middle, 0)
        send_row(later, more)
        sent_z(now)
        sent_row(now)

    half = count // 2

    def strip_refs(window, index):
        first = pl.multiple_of(index * strip // ROWS * ROWS, ROWS)
        return (
            snaps.at[window, :, pl.ds(first, ROWS), :],
            strips.at[window, kind, pl.ds(a * layers, layers)],
        )

    def strip_remote(window, index, sender, sort):
        source = snaps.at[
            window, :, pl.ds(pl.multiple_of(index * strip // ROWS * ROWS, ROWS), ROWS), :
        ]
        return pltpu.make_async_remote_copy(
            src_ref=source,
            dst_ref=strips.at[window, sort, pl.ds(sender * layers, layers)],
            send_sem=strip_send.at[window, index],
            recv_sem=strip_recv.at[window, sort, sender],
            device_id={"gz": c * half + index},
            device_id_type=MESH,
        )

    def strip_local(window, index):
        source, landed = strip_refs(window, index)
        return pltpu.make_async_copy(source, landed, strip_own.at[window])

    def start_strip(window, turn):
        index = (turn + GROUP * a + 2 * kind) % half
        target = c * half + index

        @pl.when(jnp.logical_and(target != me, turn < half))
        def _():
            strip_remote(window, index, a, kind).start()

        @pl.when(jnp.logical_and(target == me, turn < half))
        def _():
            strip_local(window, index).start()

    def sent_strips(window):
        def sent(index, carried):
            target = c * half + index

            @pl.when(target != me)
            def _():
                strip_remote(window, index, a, kind).wait_send()

            return carried

        lax.fori_loop(0, half, sent, 0)

    def wait_strip(window, sender):
        for sort in range(2):
            source = sender * GROUP + 2 * sort + me // half

            @pl.when(source != me)
            def _():
                strip_remote(window, 0, sender, sort).wait_recv()

            @pl.when(source == me)
            def _():
                strip_local(window, me % half).wait()

    lags = raw.shape[0]
    some = 16
    unit = (ROWS, breadth)
    column = lax.broadcasted_iota(jnp.int32, unit, 1)

    def first_products(block, carried):
        z = pl.ds(block * some, some)
        shot_wave = strips[0, 0, z]
        echo = strips[0, 1, z]
        light[z] = shot_wave * shot_wave
        for index in range(lags):
            back = lax.rem(2 * breadth - 2 * lag_ref[index], breadth)
            raw[index, z] = shot_wave * pltpu.roll(echo, back, 2)
        return carried

    def last_products(slab):
        def block_products(block, carried):
            z = pl.ds(slab * layers + block * some, some)
            shot_wave = strips[1, 0, z]
            echo = strips[1, 1, z]
            light[z] = light[z] + shot_wave * shot_wave
            for index in range(lags):
                lag = lag_ref[index]
                reach = jnp.abs(lag)
                inside = (column >= reach) & (column < breadth - reach)
                back = lax.rem(2 * breadth - 2 * lag, breadth)
                forth = lax.rem(breadth + lag, breadth)
                total = raw[index, z] + shot_wave * pltpu.roll(echo, back, 2)
                raw[index, z] = jnp.where(
                    inside[None], pltpu.roll(total, forth, 2), 0.0
                )
            return carried

        lax.fori_loop(0, layers // some, block_products, 0)

    if paired:
        pass_on()
    wait_load(1)
    for piece in range(PIECES):
        send_z(piece, 0)
    send_row(0)
    wait_load(0)
    wait_load(2)
    fetch(2).wait()
    fetch(3).wait()
    for index in range(3):
        for target in range(GROUP):

            @pl.when(direct(index, target))
            def _():
                load_remote(index, target, b).wait_send()

    if paired:
        passed_on()

    share = (half + SNAP_EVERY - 1) // SNAP_EVERY
    for window in range(SNAPS):

        def both(local, carried):
            whole_step(window, local)
            if window > 0:
                for part in range(share):
                    start_strip(window - 1, local * share + part)
            return carried

        lax.fori_loop(0, SNAP_EVERY, both, 0)
    lax.fori_loop(0, half, lambda turn, carried: (start_strip(SNAPS - 1, turn), carried)[1], 0)

    last = STEPS % 2

    def back_refs(sort, target):
        return (
            field.at[last, pl.ds(HALO + target * thin, thin), inner],
            outs[sort].at[:, pl.ds(pl.multiple_of(c * height, height), height), :],
        )

    def back_remote(sort, target):
        source, landed = back_refs(sort, target)
        return pltpu.make_async_remote_copy(
            src_ref=source,
            dst_ref=landed,
            send_sem=back_send.at[target],
            recv_sem=back_recv.at[sort, c],
            device_id={"gz": a * GROUP + target},
            device_id_type=MESH,
        )

    def back_arrival(sort, side):
        return pltpu.make_async_remote_copy(
            src_ref=field.at[last, pl.ds(HALO, thin), inner],
            dst_ref=outs[sort].at[:, pl.ds(side * height, height), :],
            send_sem=back_send.at[0],
            recv_sem=back_recv.at[sort, side],
            device_id={"gz": a * GROUP + 2 * sort + side},
            device_id_type=MESH,
        )

    def back_local(sort, target):
        source, landed = back_refs(sort, target)
        return pltpu.make_async_copy(source, landed, back_own.at[0])

    def each_back(remote, own):
        for sort in range(2):
            for target in range(GROUP):

                @pl.when(jnp.logical_and(kind == sort, b != target))
                def _():
                    remote(sort, target)

                if target // 2 == sort:

                    @pl.when(b == target)
                    def _():
                        own(sort, target)

    each_back(
        lambda sort, target: back_remote(sort, target).start(),
        lambda sort, target: back_local(sort, target).start(),
    )
    for sender in range(outer):
        wait_strip(0, sender)
    lax.fori_loop(0, strips.shape[2] // some, first_products, 0)

    def leaving(slab, turn):
        z = pl.ds(slab * layers, layers)
        return (
            pltpu.make_async_copy(light.at[z], light_out.at[z], out_own.at[0, turn]),
            pltpu.make_async_copy(
                raw.at[:, z], raw_out.at[:, z], out_own.at[1, turn]
            ),
        )

    def arrivals(turn, carried):
        slab = (a + turn) % outer
        wait_strip(1, slab)
        last_products(slab)
        for leave in leaving(slab, turn):
            leave.start()
        return carried

    lax.fori_loop(0, outer, arrivals, 0)
    for epoch in range(EPOCHS):
        for target in range(2):

            @pl.when(b != target)
            def _():
                edge_remote(epoch, target, b).wait_send()

    each_back(
        lambda sort, target: back_remote(sort, target).wait_send(),
        lambda sort, target: back_local(sort, target).wait(),
    )
    for sort in range(2):
        for side in range(2):

            @pl.when(b != 2 * sort + side)
            def _():
                back_arrival(sort, side).wait_recv()

    for window in range(SNAPS):
        sent_strips(window)

    def left(turn, carried):
        for leave in leaving((a + turn) % outer, turn):
            leave.wait()
        return carried

    lax.fori_loop(0, outer, left, 0)


def image_kernel(
    raw_in,
    light_in,
    src_in,
    rec_in,
    image_out,
    src_out,
    rec_out,
    raw,
    light,
    finals,
    image,
    inverse,
    light_own,
    raw_own,
    final_own,
    image_own,
):
    lags, depth = raw.shape[:2]
    unit = raw.shape[2:]
    get_light = pltpu.make_async_copy(light_in, light, light_own.at[0])
    get_light.start()
    gets = [
        pltpu.make_async_copy(source, finals.at[index], final_own.at[0, index])
        for index, source in enumerate((src_in, rec_in))
    ]
    puts = [
        pltpu.make_async_copy(finals.at[index], landed, final_own.at[1, index])
        for index, landed in enumerate((src_out, rec_out))
    ]

    def get_raw(index):
        return pltpu.make_async_copy(raw_in.at[index], raw.at[index], raw_own.at[index])

    def put_image(index):
        return pltpu.make_async_copy(
            image.at[index], image_out.at[index], image_own.at[index]
        )

    for get in gets:
        get.start()
    for index in range(lags):
        get_raw(index).start()

    pivots = []
    pivot = 0.0
    for _ in range(depth):
        pivot = 1.0 / (1.0 + 2.0 * smoothing - smoothing * smoothing * pivot)
        pivots.append(float(np.float32(pivot)))
    settled = min(z for z in range(depth) if pivots[z] == pivots[-1])
    settled = min(depth, -(-settled // 8) * 8)
    get_light.wait()

    def forward(z, pivot, carried):
        value = light[z] * pivot + (smoothing * pivot) * carried
        inverse[z] = value
        return value

    def backward(z, pivot, carried):
        value = inverse[z] + (smoothing * pivot) * carried
        inverse[z] = 1.0 / (value + damping)
        return value

    rest = (depth - settled) // 8
    value = jnp.zeros(unit, jnp.float32)
    for z in range(settled):
        value = forward(z, pivots[z], value)

    def down(turn, carried):
        for step in range(8):
            carried = forward(settled + turn * 8 + step, pivots[-1], carried)
        return carried

    lax.fori_loop(0, rest, down, value)
    for get, put in zip(gets, puts):
        get.wait()
        put.start()

    def up(turn, carried):
        for step in range(8):
            carried = backward(depth - 1 - turn * 8 - step, pivots[-1], carried)
        return carried

    value = lax.fori_loop(0, rest, up, jnp.zeros(unit, jnp.float32))
    for z in reversed(range(settled)):
        value = backward(z, pivots[z], value)

    some = 32
    for index in range(lags):
        get_raw(index).wait()

        def layers(block, carried):
            z = pl.ds(block * some, some)
            image[index, z] = (raw[index, z] * inverse[z]).astype(jnp.bfloat16)
            return carried

        lax.fori_loop(0, depth // some, layers, 0)
        put_image(index).start()
    for index in range(lags):
        put_image(index).wait()
    for put in puts:
        put.wait()


def local(
    count,
    shots,
    source_now,
    source_before,
    receiver_now,
    receiver_before,
    speed_term,
    saved_faces,
    face_steps,
    traces,
    lag_offsets,
    snap_phase,
):
    thin, wide, breadth = source_now.shape
    layers = thin * GROUP
    outer = count // GROUP
    half = count // 2
    depth = thin * count
    height = wide // 2
    strip = wide // count
    tall = height * 8 * EPOCH // breadth
    lags = lag_offsets.shape[0]
    me = lax.axis_index("gz")

    hbm = pl.BlockSpec(memory_space=pltpu.HBM)
    smem = pl.BlockSpec(memory_space=pltpu.SMEM)
    dma = pltpu.SemaphoreType.DMA
    flat = jax.ShapeDtypeStruct(source_now.shape, jnp.float32)
    raw, light, source_final, receiver_final = pl.pallas_call(
        functools.partial(wave_kernel, count, shots, strip),
        out_shape=(
            jax.ShapeDtypeStruct((lags, depth, ROWS, breadth), jnp.float32),
            jax.ShapeDtypeStruct((depth, ROWS, breadth), jnp.float32),
            flat,
            flat,
        ),
        in_specs=[smem] + [hbm] * 9,
        out_specs=(hbm, hbm, hbm, hbm),
        scratch_shapes=[
            pltpu.SMEM(snap_phase.shape, jnp.int32),
            pltpu.SMEM(face_steps.shape, jnp.int32),
            pltpu.VMEM(saved_faces.shape, jnp.float32),
            pltpu.VMEM(traces.shape, traces.dtype),
            pltpu.VMEM((2 * breadth, breadth), jnp.bfloat16),
            pltpu.VMEM((breadth, breadth), jnp.bfloat16),
            pltpu.VMEM((2, layers + 2 * HALO, height + 2 * ROWS, breadth), jnp.float32),
            pltpu.VMEM((layers, height, breadth), jnp.float32),
            pltpu.VMEM((EPOCHS, 2, thin, tall, breadth), jnp.float32),
            pltpu.VMEM((EPOCHS, layers, tall, breadth), jnp.float32),
            pltpu.VMEM((2, 2, HALO, height, breadth), jnp.float32),
            pltpu.VMEM((SNAPS, layers, height, breadth), jnp.float32),
            pltpu.VMEM((SNAPS, 2, depth, ROWS, breadth), jnp.float32),
            pltpu.VMEM((lags, depth, ROWS, breadth), jnp.float32),
            pltpu.VMEM((depth, ROWS, breadth), jnp.float32),
            dma((4,)),
            dma((3, GROUP)),
            dma((3, GROUP)),
            dma((3,)),
            dma((2,)),
            dma((2,)),
            dma((EPOCHS, 2)),
            dma((EPOCHS, GROUP)),
            dma((2, 2, PIECES)),
            dma((2, 2, PIECES)),
            dma((2,)),
            dma((2,)),
            dma((SNAPS, half)),
            dma((SNAPS, 2, outer)),
            dma((SNAPS,)),
            dma((GROUP,)),
            dma((2, 2)),
            dma((1,)),
            dma((2, outer)),
        ],
        compiler_params=pltpu.CompilerParams(
            has_side_effects=True, vmem_limit_bytes=VMEM_BYTES
        ),
        name="waves",
    )(
        lag_offsets,
        snap_phase,
        face_steps,
        source_now,
        source_before,
        receiver_now,
        receiver_before,
        speed_term,
        saved_faces,
        traces,
    )

    if strip < ROWS:
        place = (me * strip) % ROWS
        raw = lax.dynamic_slice_in_dim(raw, place, strip, 2)
        light = lax.dynamic_slice_in_dim(light, place, strip, 1)
    image_shape = (lags, depth, strip, breadth)
    return pl.pallas_call(
        image_kernel,
        out_shape=(jax.ShapeDtypeStruct(image_shape, jnp.bfloat16), flat, flat),
        in_specs=[hbm] * 4,
        out_specs=(hbm, hbm, hbm),
        scratch_shapes=[
            pltpu.VMEM(raw.shape, jnp.float32),
            pltpu.VMEM(light.shape, jnp.float32),
            pltpu.VMEM((2,) + source_now.shape, jnp.float32),
            pltpu.VMEM(image_shape, jnp.bfloat16),
            pltpu.VMEM(light.shape, jnp.float32),
            dma((1,)),
            dma((lags,)),
            dma((2, 2)),
            dma((lags,)),
        ],
        compiler_params=pltpu.CompilerParams(vmem_limit_bytes=VMEM_BYTES),
        name="images",
    )(raw, light, source_final, receiver_final)


def solution(mesh):
    return jax.shard_map(
        functools.partial(local, mesh.shape["gz"], mesh.shape["shot"]),
        mesh=mesh,
        in_specs=(
            P(("shot", "gz"), None, None),
            P(("shot", "gz"), None, None),
            P(("shot", "gz"), None, None),
            P(("shot", "gz"), None, None),
            P("gz", None, None),
            P("shot", None, "gz", None),
            P(),
            P("shot", None, None),
            P(),
            P(),
        ),
        out_specs=(
            P("shot", None, "gz", None),
            P(("shot", "gz"), None, None),
            P(("shot", "gz"), None, None),
        ),
        check_vma=False,
    )
```

```python
import functools

import jax
import jax.numpy as jnp
import numpy as np
from jax import lax
from jax.experimental import pallas as pl
from jax.experimental.pallas import tpu as pltpu
from jax.sharding import PartitionSpec as P

SNAP_EVERY = 6
SNAPS = 2
STEPS = SNAPS * SNAP_EVERY
HALO = 4
ROWS = 8
CHUNK = 4
GROUP = 4
PIECES = 4
EPOCH = 4
VMEM_BYTES = 60 * 1024 * 1024
EPOCHS = STEPS // EPOCH

stencil_weights = (-205.0 / 72.0, 8.0 / 5.0, -1.0 / 5.0, 8.0 / 315.0, -1.0 / 560.0)
damping = 0.25
smoothing = 16.0
MESH = pl.DeviceIdType.MESH


def lateral_weights(breadth):
    apart = jnp.abs(
        lax.broadcasted_iota(jnp.int32, (breadth, breadth), 0)
        - lax.broadcasted_iota(jnp.int32, (breadth, breadth), 1)
    )
    band = jnp.where(apart == 0, 3.0 * stencil_weights[0], 0.0)
    for offset in range(1, 5):
        band = jnp.where(apart == offset, stencil_weights[offset], band)
    high = band.astype(jnp.bfloat16)
    low = (band - high.astype(jnp.float32)).astype(jnp.bfloat16)
    return high, low


def wave_kernel(
    count,
    shots,
    strip,
    lag_ref,
    phase_hbm,
    order_hbm,
    src_now,
    src_old,
    rec_now,
    rec_old,
    speed,
    faces_hbm,
    traces_hbm,
    raw_out,
    light_out,
    src_out,
    rec_out,
    phase_ref,
    order_ref,
    faces,
    traces,
    weights_a,
    weights_b,
    field,
    factor,
    packed,
    edges,
    halo,
    snaps,
    strips,
    raw,
    light,
    small_own,
    load_send,
    load_recv,
    load_own,
    relay_send,
    relay_recv,
    edge_send,
    edge_recv,
    z_send,
    z_recv,
    row_send,
    row_recv,
    strip_send,
    strip_recv,
    strip_own,
    back_send,
    back_recv,
    back_own,
    out_own,
):
    me = lax.axis_index("gz")
    outer = count // GROUP
    a = me // GROUP
    b = me % GROUP
    kind = b // 2
    c = b % 2
    thin = src_now.shape[0]
    layers = thin * GROUP
    height = src_now.shape[1] // 2
    breadth = src_now.shape[2]
    inner = pl.ds(ROWS, height)
    now_of = (src_now, rec_now)
    old_of = (src_old, rec_old)
    outs = (src_out, rec_out)

    def load_refs(index, target, sender):
        rows = pl.ds(target % 2 * height, height)
        planes = pl.ds(HALO + sender * thin, thin)
        source = (speed, now_of[target // 2], old_of[target // 2])[index]
        landed = (
            factor.at[pl.ds(sender * thin, thin)],
            field.at[0, planes, inner],
            field.at[1, planes, inner],
        )[index]
        return source.at[:, rows, :], landed

    def load_remote(index, target, sender):
        source, landed = load_refs(index, target, sender)
        return pltpu.make_async_remote_copy(
            src_ref=source,
            dst_ref=landed,
            send_sem=load_send.at[index, target],
            recv_sem=load_recv.at[index, sender],
            device_id={"gz": a * GROUP + target},
            device_id_type=MESH,
        )

    def load_local(index, target):
        source, landed = load_refs(index, target, target)
        return pltpu.make_async_copy(source, landed, load_own.at[index])

    paired = shots % 2 == 0
    shot = lax.axis_index("shot")
    parity = shot % 2

    def direct(index, target):
        if index > 0 or not paired:
            return b != target
        near = jnp.logical_or(kind == target // 2, parity == target % 2)
        return jnp.logical_and(b != target, near)

    def relay(sender):
        view = factor.at[pl.ds(sender * thin, thin)]
        return pltpu.make_async_remote_copy(
            src_ref=view,
            dst_ref=view,
            send_sem=relay_send.at[sender % 2],
            recv_sem=relay_recv.at[sender % 2],
            device_id={"shot": shot + 1 - 2 * parity, "gz": me},
            device_id_type=MESH,
        )

    small = (
        (faces_hbm, faces),
        (order_hbm, order_ref),
        (phase_hbm, phase_ref),
        (traces_hbm, traces),
    )

    def fetch(index):
        source, landed = small[index]
        return pltpu.make_async_copy(source, landed, small_own.at[index])

    for index in range(3):
        for target in range(GROUP):

            @pl.when(direct(index, target))
            def _():
                load_remote(index, target, b).start()

    for index in range(len(small)):
        fetch(index).start()
    for index in range(3):
        for target in range(GROUP):

            @pl.when(b == target)
            def _():
                load_local(index, target).start()

    def wait_load(index):
        for sender in range(GROUP):

            @pl.when(b == sender)
            def _():
                load_local(index, sender).wait()

            if index > 0 or not paired:

                @pl.when(b != sender)
                def _():
                    load_remote(index, sender, sender).wait_recv()

            else:

                @pl.when(jnp.logical_and(b != sender, kind == sender // 2))
                def _():
                    load_remote(index, sender, sender).wait_recv()

                @pl.when(jnp.logical_and(kind != sender // 2, parity != c))
                def _():
                    relay(sender).wait_recv()

    def pass_on():
        for sender in range(GROUP):

            @pl.when(jnp.logical_and(kind != sender // 2, parity == c))
            def _():
                load_remote(0, sender, sender).wait_recv()
                relay(sender).start()

    def passed_on():
        for sender in range(GROUP):

            @pl.when(jnp.logical_and(kind != sender // 2, parity == c))
            def _():
                relay(sender).wait_send()

    high, low = lateral_weights(breadth)
    weights_a[pl.ds(0, breadth)] = high
    weights_a[pl.ds(breadth, breadth)] = high
    weights_b[...] = low
    fetch(0).wait()
    fetch(1).wait()

    lane = lax.broadcasted_iota(jnp.int32, (1, 1, breadth), 2)
    across = 8 * EPOCH
    groups = breadth // across
    tall = height // groups
    tiles_a_part = tall // ROWS
    for z in range(thin):
        parts = [
            pltpu.roll(faces[order_ref[step], :, z, :], 4, 0) for step in range(STEPS)
        ]
        parts.append(jnp.zeros((breadth - 8 * STEPS, 2 * height), jnp.float32))
        turned = jnp.concatenate(parts, axis=0).T
        for epoch in range(EPOCHS):
            for half in range(2):
                block = None
                for part in range(groups):
                    first = half * height + part * tall
                    moved = turned[first : first + tall]
                    turn = (across * (part - epoch)) % breadth
                    if turn:
                        moved = pltpu.roll(moved, turn, 1)
                    if block is None:
                        block = moved
                    else:
                        block = jnp.where(lane[0] >= across * part, moved, block)
                packed[epoch, half, z] = block

    def edge_remote(epoch, target, sender):
        return pltpu.make_async_remote_copy(
            src_ref=packed.at[epoch, target],
            dst_ref=edges.at[epoch, pl.ds(sender * thin, thin)],
            send_sem=edge_send.at[epoch, target],
            recv_sem=edge_recv.at[epoch, sender],
            device_id={"gz": a * GROUP + target},
            device_id_type=MESH,
        )

    for epoch in range(EPOCHS):
        for target in range(2):

            @pl.when(b != target)
            def _():
                edge_remote(epoch, target, b).start()

            @pl.when(b == target)
            def _():
                edges[epoch, pl.ds(target * thin, thin)] = packed[epoch, target]

    def wait_edge(epoch):
        for sender in range(GROUP):

            @pl.when(jnp.logical_and(kind == 0, b != sender))
            def _():
                edge_remote(epoch, 0, sender).wait_recv()

    for slot in range(2):
        for first in (0, HALO + layers):
            field[slot, pl.ds(first, HALO), inner] = jnp.zeros(
                (HALO, height, breadth), jnp.float32
            )

        @pl.when(c == 0)
        def _():
            field[slot, pl.ds(HALO, layers), pl.ds(0, ROWS)] = jnp.zeros(
                (layers, ROWS, breadth), jnp.float32
            )

        @pl.when(c == 1)
        def _():
            field[slot, pl.ds(HALO, layers), pl.ds(ROWS + height, ROWS)] = jnp.zeros(
                (layers, ROWS, breadth), jnp.float32
            )

        @pl.when(a == 0)
        def _():
            halo[0, slot] = jnp.zeros((HALO, height, breadth), jnp.float32)

        @pl.when(a == outer - 1)
        def _():
            halo[1, slot] = jnp.zeros((HALO, height, breadth), jnp.float32)

    snaps[...] = jnp.zeros(snaps.shape, jnp.float32)

    span = height // PIECES
    present = (a > 0, a < outer - 1)

    def z_copy(side, piece, slot):
        return pltpu.make_async_remote_copy(
            src_ref=field.at[
                slot,
                pl.ds((HALO, layers)[side], HALO),
                pl.ds(ROWS + piece * span, span),
            ],
            dst_ref=halo.at[1 - side, slot, :, pl.ds(piece * span, span)],
            send_sem=z_send.at[side, slot, piece],
            recv_sem=z_recv.at[1 - side, slot, piece],
            device_id={"gz": (me - GROUP, me + GROUP)[side]},
            device_id_type=MESH,
        )

    def send_z(piece, slot, also=None):
        for side in range(2):
            allowed = present[side]
            if also is not None:
                allowed = jnp.logical_and(allowed, also)

            @pl.when(allowed)
            def _():
                z_copy(side, piece, slot).start()

    def wait_z(piece, slot):
        for side in range(2):

            @pl.when(present[side])
            def _():
                z_copy(1 - side, piece, slot).wait_recv()

    def sent_z(slot):
        for side in range(2):

            @pl.when(present[side])
            def _():
                for piece in range(PIECES):
                    z_copy(side, piece, slot).wait_send()

    body = pl.ds(HALO, layers)

    def row_copy(way, slot):
        first, landed = (
            (ROWS + height - HALO, ROWS - HALO),
            (ROWS, ROWS + height),
        )[way]
        return pltpu.make_async_remote_copy(
            src_ref=field.at[slot, body, pl.ds(first, HALO)],
            dst_ref=field.at[slot, body, pl.ds(landed, HALO)],
            send_sem=row_send.at[slot],
            recv_sem=row_recv.at[slot],
            device_id={"gz": me + 1 - 2 * c},
            device_id_type=MESH,
        )

    def each_way(do, also=None):
        for way in range(2):
            allowed = c == way
            if also is not None:
                allowed = jnp.logical_and(allowed, also)

            @pl.when(allowed)
            def _():
                do(way)

    def send_row(slot, also=None):
        each_way(lambda way: row_copy(way, slot).start(), also)

    def wait_row(slot):
        each_way(lambda way: row_copy(1 - way, slot).wait_recv())

    def sent_row(slot):
        each_way(lambda way: row_copy(way, slot).wait_send())

    outside = ((lane < 4) | (lane >= breadth - 4)) & (kind == 0)
    lit = jnp.logical_and(a == 0, kind == 1)

    tiles = height // ROWS

    def partial(step, now, later, base, deep, first, many, top=False):
        planes = pl.ds(HALO + base, deep)
        start = first * ROWS
        if not isinstance(first, int):
            start = pl.multiple_of(start, ROWS)
        tall = many * ROWS
        rows = pl.ds(ROWS + start, tall)
        window = field[now, planes, pl.ds(start, tall + 2 * ROWS), :]
        center = window[:, ROWS : ROWS + tall]
        flat = center.reshape(deep * tall, breadth)
        high = flat.astype(jnp.bfloat16)
        low = (flat - high.astype(jnp.float32)).astype(jnp.bfloat16)
        lateral = jnp.dot(
            jnp.concatenate([high, low], axis=1),
            weights_a[...],
            preferred_element_type=jnp.float32,
        ) + jnp.dot(high, weights_b[...], preferred_element_type=jnp.float32)
        summed = lateral.reshape(deep, tall, breadth)
        for offset in range(1, 5):
            summed = summed + stencil_weights[offset] * (
                (
                    field[now, pl.ds(HALO + base + offset, deep), rows, :]
                    + field[now, pl.ds(HALO + base - offset, deep), rows, :]
                )
                + (
                    window[:, ROWS + offset : ROWS + offset + tall]
                    + window[:, ROWS - offset : ROWS - offset + tall]
                )
            )
        previous = field[later, planes, rows, :]
        speeds = factor[pl.ds(base, deep), pl.ds(start, tall)]
        updated = 2.0 * center - previous + speeds * summed
        placed = []
        for tile in range(many):
            place = first + tile
            inside = place % tiles_a_part * ROWS
            if not isinstance(place, int):
                inside = pl.multiple_of(inside, ROWS)
            edge = edges[step // EPOCH, pl.ds(base, deep), pl.ds(inside, ROWS)]
            turn = 3 * breadth - 4 - across * (place // tiles_a_part)
            turn = lax.rem(turn - 8 * (step % EPOCH), breadth)
            edge = pltpu.roll(edge.reshape(deep * ROWS, breadth), turn, 1)
            placed.append(edge.reshape(deep, ROWS, breadth))
        placed = placed[0] if many == 1 else jnp.concatenate(placed, axis=1)
        updated = jnp.where(outside, placed, updated)
        if top:
            trace = traces[step, pl.ds(pl.multiple_of(c * height, height), height)]
            trace = jnp.where(lit, trace.astype(jnp.float32), 0.0)
            updated = jnp.concatenate([updated[:1] + trace[None], updated[1:]], axis=0)
        return updated

    def keep(window, take, base, rows, value):
        held = snaps[window, pl.ds(base, value.shape[0]), rows]
        snaps[window, pl.ds(base, value.shape[0]), rows] = jnp.where(take, value, held)

    def complete(window, take, now, later, piece):
        rows = pl.ds(piece * span, span)
        wide = pl.ds(ROWS + piece * span, span)
        for side in range(2):
            base = (0, layers - HALO)[side]
            held = [halo[side, now, near, rows] for near in range(HALO)]
            added = []
            for near in range(HALO):
                total = None
                reach = HALO - near if side == 0 else near + 1
                for k in range(reach):
                    offset = HALO - k
                    index = near + k if side == 0 else near - k
                    term = stencil_weights[offset] * held[index]
                    total = term if total is None else total + term
                added.append(total[None])
            added = jnp.concatenate(added, axis=0)
            planes = pl.ds(HALO + base, HALO)
            added = jnp.where(outside, 0.0, factor[pl.ds(base, HALO), rows] * added)
            value = field[later, planes, wide] + added
            field[later, planes, wide] = value
            keep(window, take, base, rows, value)

    def whole_step(window, local):
        step = window * SNAP_EVERY + local
        now = lax.rem(step, 2)
        later = 1 - now
        more = step < STEPS - 1
        take = phase_ref[window] == local

        @pl.when(lax.rem(step, EPOCH) == 0)
        def _():
            wait_edge(step // EPOCH)

        wait_row(now)
        for base, top in ((0, True), (layers - HALO, False)):
            field[later, pl.ds(HALO + base, HALO), inner] = partial(
                step, now, later, base, HALO, 0, tiles, top
            )
        for piece in range(PIECES):
            wait_z(piece, now)
            complete(window, take, now, later, piece)
            send_z(piece, later, more)

        def interior(base, deep, first, many):
            start = pl.multiple_of(first * ROWS, ROWS)
            value = partial(step, now, later, base, deep, first, many)
            rows = pl.ds(ROWS + start, many * ROWS)
            field[later, pl.ds(HALO + base, deep), rows] = value
            keep(window, take, base, pl.ds(start, many * ROWS), value)

        interior(HALO, layers - 2 * HALO, (1 - c) * (tiles - 1), 1)
        send_row(later, more)

        def middle(chunk, carried):
            interior(chunk * CHUNK, CHUNK, c, tiles - 1)
            return carried

        lax.fori_loop(1, layers // CHUNK - 1, middle, 0)
        sent_z(now)
        sent_row(now)

    half = count // 2

    def strip_refs(window, index):
        first = pl.multiple_of(index * strip // ROWS * ROWS, ROWS)
        return (
            snaps.at[window, :, pl.ds(first, ROWS), :],
            strips.at[window, kind, pl.ds(a * layers, layers)],
        )

    def strip_remote(window, index, sender, sort):
        source = snaps.at[
            window, :, pl.ds(pl.multiple_of(index * strip // ROWS * ROWS, ROWS), ROWS), :
        ]
        return pltpu.make_async_remote_copy(
            src_ref=source,
            dst_ref=strips.at[window, sort, pl.ds(sender * layers, layers)],
            send_sem=strip_send.at[window, index],
            recv_sem=strip_recv.at[window, sort, sender],
            device_id={"gz": c * half + index},
            device_id_type=MESH,
        )

    def strip_local(window, index):
        source, landed = strip_refs(window, index)
        return pltpu.make_async_copy(source, landed, strip_own.at[window])

    def start_strip(window, turn):
        index = (turn + GROUP * a + 2 * kind) % half
        target = c * half + index

        @pl.when(jnp.logical_and(target != me, turn < half))
        def _():
            strip_remote(window, index, a, kind).start()

        @pl.when(jnp.logical_and(target == me, turn < half))
        def _():
            strip_local(window, index).start()

    def sent_strips(window):
        def sent(index, carried):
            target = c * half + index

            @pl.when(target != me)
            def _():
                strip_remote(window, index, a, kind).wait_send()

            return carried

        lax.fori_loop(0, half, sent, 0)

    def wait_strip(window, sender):
        for sort in range(2):
            source = sender * GROUP + 2 * sort + me // half

            @pl.when(source != me)
            def _():
                strip_remote(window, 0, sender, sort).wait_recv()

            @pl.when(source == me)
            def _():
                strip_local(window, me % half).wait()

    lags = raw.shape[0]
    some = 16
    unit = (ROWS, breadth)
    column = lax.broadcasted_iota(jnp.int32, unit, 1)

    def first_products(block, carried):
        z = pl.ds(block * some, some)
        shot_wave = strips[0, 0, z]
        echo = strips[0, 1, z]
        light[z] = shot_wave * shot_wave
        for index in range(lags):
            back = lax.rem(2 * breadth - 2 * lag_ref[index], breadth)
            raw[index, z] = shot_wave * pltpu.roll(echo, back, 2)
        return carried

    def last_products(slab):
        def block_products(block, carried):
            z = pl.ds(slab * layers + block * some, some)
            shot_wave = strips[1, 0, z]
            echo = strips[1, 1, z]
            light[z] = light[z] + shot_wave * shot_wave
            for index in range(lags):
                lag = lag_ref[index]
                reach = jnp.abs(lag)
                inside = (column >= reach) & (column < breadth - reach)
                back = lax.rem(2 * breadth - 2 * lag, breadth)
                forth = lax.rem(breadth + lag, breadth)
                total = raw[index, z] + shot_wave * pltpu.roll(echo, back, 2)
                raw[index, z] = jnp.where(
                    inside[None], pltpu.roll(total, forth, 2), 0.0
                )
            return carried

        lax.fori_loop(0, layers // some, block_products, 0)

    if paired:
        pass_on()
    wait_load(1)
    for piece in range(PIECES):
        send_z(piece, 0)
    send_row(0)
    wait_load(0)
    wait_load(2)
    fetch(2).wait()
    fetch(3).wait()
    for index in range(3):
        for target in range(GROUP):

            @pl.when(direct(index, target))
            def _():
                load_remote(index, target, b).wait_send()

    if paired:
        passed_on()

    share = (half + SNAP_EVERY - 1) // SNAP_EVERY
    for window in range(SNAPS):

        def both(local, carried):
            whole_step(window, local)
            if window > 0:
                for part in range(share):
                    start_strip(window - 1, local * share + part)
            return carried

        lax.fori_loop(0, SNAP_EVERY, both, 0)
    lax.fori_loop(0, half, lambda turn, carried: (start_strip(SNAPS - 1, turn), carried)[1], 0)

    last = STEPS % 2

    def back_refs(sort, target):
        return (
            field.at[last, pl.ds(HALO + target * thin, thin), inner],
            outs[sort].at[:, pl.ds(pl.multiple_of(c * height, height), height), :],
        )

    def back_remote(sort, target):
        source, landed = back_refs(sort, target)
        return pltpu.make_async_remote_copy(
            src_ref=source,
            dst_ref=landed,
            send_sem=back_send.at[target],
            recv_sem=back_recv.at[sort, c],
            device_id={"gz": a * GROUP + target},
            device_id_type=MESH,
        )

    def back_arrival(sort, side):
        return pltpu.make_async_remote_copy(
            src_ref=field.at[last, pl.ds(HALO, thin), inner],
            dst_ref=outs[sort].at[:, pl.ds(side * height, height), :],
            send_sem=back_send.at[0],
            recv_sem=back_recv.at[sort, side],
            device_id={"gz": a * GROUP + 2 * sort + side},
            device_id_type=MESH,
        )

    def back_local(sort, target):
        source, landed = back_refs(sort, target)
        return pltpu.make_async_copy(source, landed, back_own.at[0])

    def each_back(remote, own):
        for sort in range(2):
            for target in range(GROUP):

                @pl.when(jnp.logical_and(kind == sort, b != target))
                def _():
                    remote(sort, target)

                if target // 2 == sort:

                    @pl.when(b == target)
                    def _():
                        own(sort, target)

    each_back(
        lambda sort, target: back_remote(sort, target).start(),
        lambda sort, target: back_local(sort, target).start(),
    )
    for sender in range(outer):
        wait_strip(0, sender)
    lax.fori_loop(0, strips.shape[2] // some, first_products, 0)

    def leaving(slab, turn):
        z = pl.ds(slab * layers, layers)
        return (
            pltpu.make_async_copy(light.at[z], light_out.at[z], out_own.at[0, turn]),
            pltpu.make_async_copy(
                raw.at[:, z], raw_out.at[:, z], out_own.at[1, turn]
            ),
        )

    def arrivals(turn, carried):
        slab = (a + turn) % outer
        wait_strip(1, slab)
        last_products(slab)
        for leave in leaving(slab, turn):
            leave.start()
        return carried

    lax.fori_loop(0, outer, arrivals, 0)
    for epoch in range(EPOCHS):
        for target in range(2):

            @pl.when(b != target)
            def _():
                edge_remote(epoch, target, b).wait_send()

    each_back(
        lambda sort, target: back_remote(sort, target).wait_send(),
        lambda sort, target: back_local(sort, target).wait(),
    )
    for sort in range(2):
        for side in range(2):

            @pl.when(b != 2 * sort + side)
            def _():
                back_arrival(sort, side).wait_recv()

    for window in range(SNAPS):
        sent_strips(window)

    def left(turn, carried):
        for leave in leaving((a + turn) % outer, turn):
            leave.wait()
        return carried

    lax.fori_loop(0, outer, left, 0)


def image_kernel(
    raw_in,
    light_in,
    src_in,
    rec_in,
    image_out,
    src_out,
    rec_out,
    raw,
    light,
    finals,
    image,
    inverse,
    light_own,
    raw_own,
    final_own,
    image_own,
):
    lags, depth = raw.shape[:2]
    unit = raw.shape[2:]
    get_light = pltpu.make_async_copy(light_in, light, light_own.at[0])
    get_light.start()
    gets = [
        pltpu.make_async_copy(source, finals.at[index], final_own.at[0, index])
        for index, source in enumerate((src_in, rec_in))
    ]
    puts = [
        pltpu.make_async_copy(finals.at[index], landed, final_own.at[1, index])
        for index, landed in enumerate((src_out, rec_out))
    ]

    def get_raw(index):
        return pltpu.make_async_copy(raw_in.at[index], raw.at[index], raw_own.at[index])

    def put_image(index):
        return pltpu.make_async_copy(
            image.at[index], image_out.at[index], image_own.at[index]
        )

    for get in gets:
        get.start()
    for index in range(lags):
        get_raw(index).start()

    pivots = []
    pivot = 0.0
    for _ in range(depth):
        pivot = 1.0 / (1.0 + 2.0 * smoothing - smoothing * smoothing * pivot)
        pivots.append(float(np.float32(pivot)))
    settled = min(z for z in range(depth) if pivots[z] == pivots[-1])
    settled = min(depth, -(-settled // 8) * 8)
    get_light.wait()

    def forward(z, pivot, carried):
        value = light[z] * pivot + (smoothing * pivot) * carried
        inverse[z] = value
        return value

    def backward(z, pivot, carried):
        value = inverse[z] + (smoothing * pivot) * carried
        inverse[z] = 1.0 / (value + damping)
        return value

    rest = (depth - settled) // 8
    value = jnp.zeros(unit, jnp.float32)
    for z in range(settled):
        value = forward(z, pivots[z], value)

    def down(turn, carried):
        for step in range(8):
            carried = forward(settled + turn * 8 + step, pivots[-1], carried)
        return carried

    lax.fori_loop(0, rest, down, value)
    for get, put in zip(gets, puts):
        get.wait()
        put.start()

    def up(turn, carried):
        for step in range(8):
            carried = backward(depth - 1 - turn * 8 - step, pivots[-1], carried)
        return carried

    value = lax.fori_loop(0, rest, up, jnp.zeros(unit, jnp.float32))
    for z in reversed(range(settled)):
        value = backward(z, pivots[z], value)

    some = 32
    for index in range(lags):
        get_raw(index).wait()

        def layers(block, carried):
            z = pl.ds(block * some, some)
            image[index, z] = (raw[index, z] * inverse[z]).astype(jnp.bfloat16)
            return carried

        lax.fori_loop(0, depth // some, layers, 0)
        put_image(index).start()
    for index in range(lags):
        put_image(index).wait()
    for put in puts:
        put.wait()


def local(
    count,
    shots,
    source_now,
    source_before,
    receiver_now,
    receiver_before,
    speed_term,
    saved_faces,
    face_steps,
    traces,
    lag_offsets,
    snap_phase,
):
    thin, wide, breadth = source_now.shape
    layers = thin * GROUP
    outer = count // GROUP
    half = count // 2
    depth = thin * count
    height = wide // 2
    strip = wide // count
    tall = height * 8 * EPOCH // breadth
    lags = lag_offsets.shape[0]
    me = lax.axis_index("gz")

    hbm = pl.BlockSpec(memory_space=pltpu.HBM)
    smem = pl.BlockSpec(memory_space=pltpu.SMEM)
    dma = pltpu.SemaphoreType.DMA
    flat = jax.ShapeDtypeStruct(source_now.shape, jnp.float32)
    raw, light, source_final, receiver_final = pl.pallas_call(
        functools.partial(wave_kernel, count, shots, strip),
        out_shape=(
            jax.ShapeDtypeStruct((lags, depth, ROWS, breadth), jnp.float32),
            jax.ShapeDtypeStruct((depth, ROWS, breadth), jnp.float32),
            flat,
            flat,
        ),
        in_specs=[smem] + [hbm] * 9,
        out_specs=(hbm, hbm, hbm, hbm),
        scratch_shapes=[
            pltpu.SMEM(snap_phase.shape, jnp.int32),
            pltpu.SMEM(face_steps.shape, jnp.int32),
            pltpu.VMEM(saved_faces.shape, jnp.float32),
            pltpu.VMEM(traces.shape, traces.dtype),
            pltpu.VMEM((2 * breadth, breadth), jnp.bfloat16),
            pltpu.VMEM((breadth, breadth), jnp.bfloat16),
            pltpu.VMEM((2, layers + 2 * HALO, height + 2 * ROWS, breadth), jnp.float32),
            pltpu.VMEM((layers, height, breadth), jnp.float32),
            pltpu.VMEM((EPOCHS, 2, thin, tall, breadth), jnp.float32),
            pltpu.VMEM((EPOCHS, layers, tall, breadth), jnp.float32),
            pltpu.VMEM((2, 2, HALO, height, breadth), jnp.float32),
            pltpu.VMEM((SNAPS, layers, height, breadth), jnp.float32),
            pltpu.VMEM((SNAPS, 2, depth, ROWS, breadth), jnp.float32),
            pltpu.VMEM((lags, depth, ROWS, breadth), jnp.float32),
            pltpu.VMEM((depth, ROWS, breadth), jnp.float32),
            dma((4,)),
            dma((3, GROUP)),
            dma((3, GROUP)),
            dma((3,)),
            dma((2,)),
            dma((2,)),
            dma((EPOCHS, 2)),
            dma((EPOCHS, GROUP)),
            dma((2, 2, PIECES)),
            dma((2, 2, PIECES)),
            dma((2,)),
            dma((2,)),
            dma((SNAPS, half)),
            dma((SNAPS, 2, outer)),
            dma((SNAPS,)),
            dma((GROUP,)),
            dma((2, 2)),
            dma((1,)),
            dma((2, outer)),
        ],
        compiler_params=pltpu.CompilerParams(
            has_side_effects=True, vmem_limit_bytes=VMEM_BYTES
        ),
        name="waves",
    )(
        lag_offsets,
        snap_phase,
        face_steps,
        source_now,
        source_before,
        receiver_now,
        receiver_before,
        speed_term,
        saved_faces,
        traces,
    )

    if strip < ROWS:
        place = (me * strip) % ROWS
        raw = lax.dynamic_slice_in_dim(raw, place, strip, 2)
        light = lax.dynamic_slice_in_dim(light, place, strip, 1)
    image_shape = (lags, depth, strip, breadth)
    return pl.pallas_call(
        image_kernel,
        out_shape=(jax.ShapeDtypeStruct(image_shape, jnp.bfloat16), flat, flat),
        in_specs=[hbm] * 4,
        out_specs=(hbm, hbm, hbm),
        scratch_shapes=[
            pltpu.VMEM(raw.shape, jnp.float32),
            pltpu.VMEM(light.shape, jnp.float32),
            pltpu.VMEM((2,) + source_now.shape, jnp.float32),
            pltpu.VMEM(image_shape, jnp.bfloat16),
            pltpu.VMEM(light.shape, jnp.float32),
            dma((1,)),
            dma((lags,)),
            dma((2, 2)),
            dma((lags,)),
        ],
        compiler_params=pltpu.CompilerParams(vmem_limit_bytes=VMEM_BYTES),
        name="images",
    )(raw, light, source_final, receiver_final)


def solution(mesh):
    return jax.shard_map(
        functools.partial(local, mesh.shape["gz"], mesh.shape["shot"]),
        mesh=mesh,
        in_specs=(
            P(("shot", "gz"), None, None),
            P(("shot", "gz"), None, None),
            P(("shot", "gz"), None, None),
            P(("shot", "gz"), None, None),
            P("gz", None, None),
            P("shot", None, "gz", None),
            P(),
            P("shot", None, None),
            P(),
            P(),
        ),
        out_specs=(
            P("shot", None, "gz", None),
            P(("shot", "gz"), None, None),
            P(("shot", "gz"), None, None),
        ),
        check_vma=False,
    )
```

```python
import functools

import jax
import jax.numpy as jnp
import numpy as np
from jax import lax
from jax.experimental import pallas as pl
from jax.experimental.pallas import tpu as pltpu
from jax.sharding import PartitionSpec as P

SNAP_EVERY = 6
SNAPS = 2
STEPS = SNAPS * SNAP_EVERY
HALO = 4
ROWS = 8
CHUNK = 4
GROUP = 4
PIECES = 4
EPOCH = 4
VMEM_BYTES = 60 * 1024 * 1024
EPOCHS = STEPS // EPOCH

stencil_weights = (-205.0 / 72.0, 8.0 / 5.0, -1.0 / 5.0, 8.0 / 315.0, -1.0 / 560.0)
damping = 0.25
smoothing = 16.0
MESH = pl.DeviceIdType.MESH


def lateral_weights(breadth):
    apart = jnp.abs(
        lax.broadcasted_iota(jnp.int32, (breadth, breadth), 0)
        - lax.broadcasted_iota(jnp.int32, (breadth, breadth), 1)
    )
    band = jnp.where(apart == 0, 3.0 * stencil_weights[0], 0.0)
    for offset in range(1, 5):
        band = jnp.where(apart == offset, stencil_weights[offset], band)
    high = band.astype(jnp.bfloat16)
    low = (band - high.astype(jnp.float32)).astype(jnp.bfloat16)
    return high, low


def close_barrier(outer):
    return outer <= SNAP_EVERY


def wave_kernel(
    count,
    shots,
    strip,
    lag_ref,
    phase_hbm,
    order_hbm,
    src_now,
    src_old,
    rec_now,
    rec_old,
    speed,
    faces_hbm,
    traces_hbm,
    raw_out,
    light_out,
    src_out,
    rec_out,
    phase_ref,
    order_ref,
    faces,
    traces,
    weights_a,
    weights_b,
    field,
    factor,
    packed,
    edges,
    halo,
    snaps,
    strips,
    raw,
    light,
    small_own,
    load_send,
    load_recv,
    load_own,
    relay_send,
    relay_recv,
    edge_send,
    edge_recv,
    z_send,
    z_recv,
    row_send,
    row_recv,
    strip_send,
    strip_recv,
    strip_own,
    back_send,
    back_recv,
    back_own,
    out_own,
):
    me = lax.axis_index("gz")
    outer = count // GROUP
    a = me // GROUP
    b = me % GROUP
    kind = b // 2
    c = b % 2
    thin = src_now.shape[0]
    layers = thin * GROUP
    height = src_now.shape[1] // 2
    breadth = src_now.shape[2]
    inner = pl.ds(ROWS, height)
    now_of = (src_now, rec_now)
    old_of = (src_old, rec_old)
    outs = (src_out, rec_out)

    paired = shots % 2 == 0
    shot = lax.axis_index("shot")
    parity = shot % 2
    other_shot = {"shot": shot + 1 - 2 * parity, "gz": me}

    if close_barrier(outer):
        barrier = pltpu.get_barrier_semaphore()

        def greet(device):
            pl.semaphore_signal(barrier, inc=1, device_id=device, device_id_type=MESH)

        for shift in range(1, GROUP):
            greet({"gz": a * GROUP + (b + shift) % GROUP})
        if paired:
            greet(other_shot)

        @pl.when(a > 0)
        def _():
            greet({"gz": me - GROUP})

        @pl.when(a < outer - 1)
        def _():
            greet({"gz": me + GROUP})

        beside = (a > 0, a < outer - 1)
        for count_beside, met in (
            (2, jnp.logical_and(*beside)),
            (1, beside[0] != beside[1]),
            (0, jnp.logical_not(jnp.logical_or(*beside))),
        ):

            @pl.when(met)
            def _():
                pl.semaphore_wait(barrier, GROUP - 1 + paired + count_beside)

    def load_refs(index, target, sender):
        rows = pl.ds(target % 2 * height, height)
        planes = pl.ds(HALO + sender * thin, thin)
        source = (speed, now_of[target // 2], old_of[target // 2])[index]
        landed = (
            factor.at[pl.ds(sender * thin, thin)],
            field.at[0, planes, inner],
            field.at[1, planes, inner],
        )[index]
        return source.at[:, rows, :], landed

    def load_remote(index, target, sender):
        source, landed = load_refs(index, target, sender)
        return pltpu.make_async_remote_copy(
            src_ref=source,
            dst_ref=landed,
            send_sem=load_send.at[index, target],
            recv_sem=load_recv.at[index, sender],
            device_id={"gz": a * GROUP + target},
            device_id_type=MESH,
        )

    def load_local(index, target):
        source, landed = load_refs(index, target, target)
        return pltpu.make_async_copy(source, landed, load_own.at[index])

    def direct(index, target):
        if index > 0 or not paired:
            return b != target
        near = jnp.logical_or(kind == target // 2, parity == target % 2)
        return jnp.logical_and(b != target, near)

    def relay(sender):
        view = factor.at[pl.ds(sender * thin, thin)]
        return pltpu.make_async_remote_copy(
            src_ref=view,
            dst_ref=view,
            send_sem=relay_send.at[sender % 2],
            recv_sem=relay_recv.at[sender % 2],
            device_id=other_shot,
            device_id_type=MESH,
        )

    small = (
        (faces_hbm, faces),
        (order_hbm, order_ref),
        (phase_hbm, phase_ref),
        (traces_hbm, traces),
    )

    def fetch(index):
        source, landed = small[index]
        return pltpu.make_async_copy(source, landed, small_own.at[index])

    for index in range(3):
        for target in range(GROUP):

            @pl.when(direct(index, target))
            def _():
                load_remote(index, target, b).start()

    for index in range(len(small)):
        fetch(index).start()
    for index in range(3):
        for target in range(GROUP):

            @pl.when(b == target)
            def _():
                load_local(index, target).start()

    def wait_load(index):
        for sender in range(GROUP):

            @pl.when(b == sender)
            def _():
                load_local(index, sender).wait()

            if index > 0 or not paired:

                @pl.when(b != sender)
                def _():
                    load_remote(index, sender, sender).wait_recv()

            else:

                @pl.when(jnp.logical_and(b != sender, kind == sender // 2))
                def _():
                    load_remote(index, sender, sender).wait_recv()

                @pl.when(jnp.logical_and(kind != sender // 2, parity != c))
                def _():
                    relay(sender).wait_recv()

    def pass_on():
        for sender in range(GROUP):

            @pl.when(jnp.logical_and(kind != sender // 2, parity == c))
            def _():
                load_remote(0, sender, sender).wait_recv()
                relay(sender).start()

    def passed_on():
        for sender in range(GROUP):

            @pl.when(jnp.logical_and(kind != sender // 2, parity == c))
            def _():
                relay(sender).wait_send()

    high, low = lateral_weights(breadth)
    weights_a[pl.ds(0, breadth)] = high
    weights_a[pl.ds(breadth, breadth)] = high
    weights_b[...] = low
    fetch(0).wait()
    fetch(1).wait()

    lane = lax.broadcasted_iota(jnp.int32, (1, 1, breadth), 2)
    across = 8 * EPOCH
    groups = breadth // across
    tall = height // groups
    tiles_a_part = tall // ROWS
    for z in range(thin):
        parts = [
            pltpu.roll(faces[order_ref[step], :, z, :], 4, 0) for step in range(STEPS)
        ]
        parts.append(jnp.zeros((breadth - 8 * STEPS, 2 * height), jnp.float32))
        turned = jnp.concatenate(parts, axis=0).T
        for epoch in range(EPOCHS):
            for half in range(2):
                block = None
                for part in range(groups):
                    first = half * height + part * tall
                    moved = turned[first : first + tall]
                    turn = (across * (part - epoch)) % breadth
                    if turn:
                        moved = pltpu.roll(moved, turn, 1)
                    if block is None:
                        block = moved
                    else:
                        block = jnp.where(lane[0] >= across * part, moved, block)
                packed[epoch, half, z] = block

    def edge_remote(epoch, target, sender):
        return pltpu.make_async_remote_copy(
            src_ref=packed.at[epoch, target],
            dst_ref=edges.at[epoch, pl.ds(sender * thin, thin)],
            send_sem=edge_send.at[epoch, target],
            recv_sem=edge_recv.at[epoch, sender],
            device_id={"gz": a * GROUP + target},
            device_id_type=MESH,
        )

    for epoch in range(EPOCHS):
        for target in range(2):

            @pl.when(b != target)
            def _():
                edge_remote(epoch, target, b).start()

            @pl.when(b == target)
            def _():
                edges[epoch, pl.ds(target * thin, thin)] = packed[epoch, target]

    def wait_edge(epoch):
        for sender in range(GROUP):

            @pl.when(jnp.logical_and(kind == 0, b != sender))
            def _():
                edge_remote(epoch, 0, sender).wait_recv()

    for slot in range(2):
        for first in (0, HALO + layers):
            field[slot, pl.ds(first, HALO), inner] = jnp.zeros(
                (HALO, height, breadth), jnp.float32
            )

        @pl.when(c == 0)
        def _():
            field[slot, pl.ds(HALO, layers), pl.ds(0, ROWS)] = jnp.zeros(
                (layers, ROWS, breadth), jnp.float32
            )

        @pl.when(c == 1)
        def _():
            field[slot, pl.ds(HALO, layers), pl.ds(ROWS + height, ROWS)] = jnp.zeros(
                (layers, ROWS, breadth), jnp.float32
            )

        @pl.when(a == 0)
        def _():
            halo[0, slot] = jnp.zeros((HALO, height, breadth), jnp.float32)

        @pl.when(a == outer - 1)
        def _():
            halo[1, slot] = jnp.zeros((HALO, height, breadth), jnp.float32)

    snaps[...] = jnp.zeros(snaps.shape, jnp.float32)

    span = height // PIECES
    present = (a > 0, a < outer - 1)

    def z_copy(side, piece, slot):
        return pltpu.make_async_remote_copy(
            src_ref=field.at[
                slot,
                pl.ds((HALO, layers)[side], HALO),
                pl.ds(ROWS + piece * span, span),
            ],
            dst_ref=halo.at[1 - side, slot, :, pl.ds(piece * span, span)],
            send_sem=z_send.at[side, slot, piece],
            recv_sem=z_recv.at[1 - side, slot, piece],
            device_id={"gz": (me - GROUP, me + GROUP)[side]},
            device_id_type=MESH,
        )

    def send_z(piece, slot, also=None):
        for side in range(2):
            allowed = present[side]
            if also is not None:
                allowed = jnp.logical_and(allowed, also)

            @pl.when(allowed)
            def _():
                z_copy(side, piece, slot).start()

    def wait_z(piece, slot):
        for side in range(2):

            @pl.when(present[side])
            def _():
                z_copy(1 - side, piece, slot).wait_recv()

    def sent_z(slot):
        for side in range(2):

            @pl.when(present[side])
            def _():
                for piece in range(PIECES):
                    z_copy(side, piece, slot).wait_send()

    body = pl.ds(HALO, layers)

    def row_copy(way, slot):
        first, landed = (
            (ROWS + height - HALO, ROWS - HALO),
            (ROWS, ROWS + height),
        )[way]
        return pltpu.make_async_remote_copy(
            src_ref=field.at[slot, body, pl.ds(first, HALO)],
            dst_ref=field.at[slot, body, pl.ds(landed, HALO)],
            send_sem=row_send.at[slot],
            recv_sem=row_recv.at[slot],
            device_id={"gz": me + 1 - 2 * c},
            device_id_type=MESH,
        )

    def each_way(do, also=None):
        for way in range(2):
            allowed = c == way
            if also is not None:
                allowed = jnp.logical_and(allowed, also)

            @pl.when(allowed)
            def _():
                do(way)

    def send_row(slot, also=None):
        each_way(lambda way: row_copy(way, slot).start(), also)

    def wait_row(slot):
        each_way(lambda way: row_copy(1 - way, slot).wait_recv())

    def sent_row(slot):
        each_way(lambda way: row_copy(way, slot).wait_send())

    outside = ((lane < 4) | (lane >= breadth - 4)) & (kind == 0)
    lit = jnp.logical_and(a == 0, kind == 1)

    tiles = height // ROWS

    def partial(step, now, later, base, deep, first, many, top=False):
        planes = pl.ds(HALO + base, deep)
        start = first * ROWS
        if not isinstance(first, int):
            start = pl.multiple_of(start, ROWS)
        tall = many * ROWS
        rows = pl.ds(ROWS + start, tall)
        window = field[now, planes, pl.ds(start, tall + 2 * ROWS), :]
        center = window[:, ROWS : ROWS + tall]
        flat = center.reshape(deep * tall, breadth)
        high = flat.astype(jnp.bfloat16)
        low = (flat - high.astype(jnp.float32)).astype(jnp.bfloat16)
        lateral = jnp.dot(
            jnp.concatenate([high, low], axis=1),
            weights_a[...],
            preferred_element_type=jnp.float32,
        ) + jnp.dot(high, weights_b[...], preferred_element_type=jnp.float32)
        summed = lateral.reshape(deep, tall, breadth)
        for offset in range(1, 5):
            summed = summed + stencil_weights[offset] * (
                (
                    field[now, pl.ds(HALO + base + offset, deep), rows, :]
                    + field[now, pl.ds(HALO + base - offset, deep), rows, :]
                )
                + (
                    window[:, ROWS + offset : ROWS + offset + tall]
                    + window[:, ROWS - offset : ROWS - offset + tall]
                )
            )
        previous = field[later, planes, rows, :]
        speeds = factor[pl.ds(base, deep), pl.ds(start, tall)]
        updated = 2.0 * center - previous + speeds * summed
        placed = []
        for tile in range(many):
            place = first + tile
            inside = place % tiles_a_part * ROWS
            if not isinstance(place, int):
                inside = pl.multiple_of(inside, ROWS)
            edge = edges[step // EPOCH, pl.ds(base, deep), pl.ds(inside, ROWS)]
            turn = 3 * breadth - 4 - across * (place // tiles_a_part)
            turn = lax.rem(turn - 8 * (step % EPOCH), breadth)
            edge = pltpu.roll(edge.reshape(deep * ROWS, breadth), turn, 1)
            placed.append(edge.reshape(deep, ROWS, breadth))
        placed = placed[0] if many == 1 else jnp.concatenate(placed, axis=1)
        updated = jnp.where(outside, placed, updated)
        if top:
            trace = traces[step, pl.ds(pl.multiple_of(c * height, height), height)]
            trace = jnp.where(lit, trace.astype(jnp.float32), 0.0)
            updated = jnp.concatenate([updated[:1] + trace[None], updated[1:]], axis=0)
        return updated

    def keep(window, take, base, rows, value):
        held = snaps[window, pl.ds(base, value.shape[0]), rows]
        snaps[window, pl.ds(base, value.shape[0]), rows] = jnp.where(take, value, held)

    def complete(window, take, now, later, piece):
        rows = pl.ds(piece * span, span)
        wide = pl.ds(ROWS + piece * span, span)
        for side in range(2):
            base = (0, layers - HALO)[side]
            held = [halo[side, now, near, rows] for near in range(HALO)]
            added = []
            for near in range(HALO):
                total = None
                reach = HALO - near if side == 0 else near + 1
                for k in range(reach):
                    offset = HALO - k
                    index = near + k if side == 0 else near - k
                    term = stencil_weights[offset] * held[index]
                    total = term if total is None else total + term
                added.append(total[None])
            added = jnp.concatenate(added, axis=0)
            planes = pl.ds(HALO + base, HALO)
            added = jnp.where(outside, 0.0, factor[pl.ds(base, HALO), rows] * added)
            value = field[later, planes, wide] + added
            field[later, planes, wide] = value
            keep(window, take, base, rows, value)

    def whole_step(window, local):
        step = window * SNAP_EVERY + local
        now = lax.rem(step, 2)
        later = 1 - now
        more = step < STEPS - 1
        take = phase_ref[window] == local

        @pl.when(lax.rem(step, EPOCH) == 0)
        def _():
            wait_edge(step // EPOCH)

        wait_row(now)
        for base, top in ((0, True), (layers - HALO, False)):
            field[later, pl.ds(HALO + base, HALO), inner] = partial(
                step, now, later, base, HALO, 0, tiles, top
            )
        for piece in range(PIECES):
            wait_z(piece, now)
            complete(window, take, now, later, piece)
            send_z(piece, later, more)

        def interior(base, deep, first, many):
            start = pl.multiple_of(first * ROWS, ROWS)
            value = partial(step, now, later, base, deep, first, many)
            rows = pl.ds(ROWS + start, many * ROWS)
            field[later, pl.ds(HALO + base, deep), rows] = value
            keep(window, take, base, pl.ds(start, many * ROWS), value)

        interior(HALO, layers - 2 * HALO, (1 - c) * (tiles - 1), 1)
        send_row(later, more)

        def middle(chunk, carried):
            interior(chunk * CHUNK, CHUNK, c, tiles - 1)
            return carried

        lax.fori_loop(1, layers // CHUNK - 1, middle, 0)
        sent_z(now)
        sent_row(now)

    half = count // 2

    def strip_refs(window, index):
        first = pl.multiple_of(index * strip // ROWS * ROWS, ROWS)
        return (
            snaps.at[window, :, pl.ds(first, ROWS), :],
            strips.at[window, kind, pl.ds(a * layers, layers)],
        )

    def strip_remote(window, index, sender, sort):
        source = snaps.at[
            window, :, pl.ds(pl.multiple_of(index * strip // ROWS * ROWS, ROWS), ROWS), :
        ]
        return pltpu.make_async_remote_copy(
            src_ref=source,
            dst_ref=strips.at[window, sort, pl.ds(sender * layers, layers)],
            send_sem=strip_send.at[window, index],
            recv_sem=strip_recv.at[window, sort, sender],
            device_id={"gz": c * half + index},
            device_id_type=MESH,
        )

    def strip_local(window, index):
        source, landed = strip_refs(window, index)
        return pltpu.make_async_copy(source, landed, strip_own.at[window])

    def start_strip(window, turn):
        index = (turn + GROUP * a + 2 * kind) % half
        target = c * half + index

        @pl.when(jnp.logical_and(target != me, turn < half))
        def _():
            strip_remote(window, index, a, kind).start()

        @pl.when(jnp.logical_and(target == me, turn < half))
        def _():
            strip_local(window, index).start()

    def sent_strips(window):
        def sent(index, carried):
            target = c * half + index

            @pl.when(target != me)
            def _():
                strip_remote(window, index, a, kind).wait_send()

            return carried

        lax.fori_loop(0, half, sent, 0)

    def wait_strip(window, sender):
        for sort in range(2):
            source = sender * GROUP + 2 * sort + me // half

            @pl.when(source != me)
            def _():
                strip_remote(window, 0, sender, sort).wait_recv()

            @pl.when(source == me)
            def _():
                strip_local(window, me % half).wait()

    lags = raw.shape[0]
    some = 16
    unit = (ROWS, breadth)
    column = lax.broadcasted_iota(jnp.int32, unit, 1)

    def first_products(block, carried):
        z = pl.ds(block * some, some)
        shot_wave = strips[0, 0, z]
        echo = strips[0, 1, z]
        light[z] = shot_wave * shot_wave
        for index in range(lags):
            back = lax.rem(2 * breadth - 2 * lag_ref[index], breadth)
            raw[index, z] = shot_wave * pltpu.roll(echo, back, 2)
        return carried

    def last_products(slab):
        def block_products(block, carried):
            z = pl.ds(slab * layers + block * some, some)
            shot_wave = strips[1, 0, z]
            echo = strips[1, 1, z]
            light[z] = light[z] + shot_wave * shot_wave
            for index in range(lags):
                lag = lag_ref[index]
                reach = jnp.abs(lag)
                inside = (column >= reach) & (column < breadth - reach)
                back = lax.rem(2 * breadth - 2 * lag, breadth)
                forth = lax.rem(breadth + lag, breadth)
                total = raw[index, z] + shot_wave * pltpu.roll(echo, back, 2)
                raw[index, z] = jnp.where(
                    inside[None], pltpu.roll(total, forth, 2), 0.0
                )
            return carried

        lax.fori_loop(0, layers // some, block_products, 0)

    if paired:
        pass_on()
    wait_load(1)
    for piece in range(PIECES):
        send_z(piece, 0)
    send_row(0)
    wait_load(0)
    wait_load(2)
    fetch(2).wait()
    fetch(3).wait()
    for index in range(3):
        for target in range(GROUP):

            @pl.when(direct(index, target))
            def _():
                load_remote(index, target, b).wait_send()

    if paired:
        passed_on()

    share = (half + SNAP_EVERY - 1) // SNAP_EVERY
    for window in range(SNAPS):

        def both(local, carried):
            whole_step(window, local)
            if window > 0:
                for part in range(share):
                    start_strip(window - 1, local * share + part)
            return carried

        lax.fori_loop(0, SNAP_EVERY, both, 0)
    lax.fori_loop(0, half, lambda turn, carried: (start_strip(SNAPS - 1, turn), carried)[1], 0)

    last = STEPS % 2

    def back_refs(sort, target):
        return (
            field.at[last, pl.ds(HALO + target * thin, thin), inner],
            outs[sort].at[:, pl.ds(pl.multiple_of(c * height, height), height), :],
        )

    def back_remote(sort, target):
        source, landed = back_refs(sort, target)
        return pltpu.make_async_remote_copy(
            src_ref=source,
            dst_ref=landed,
            send_sem=back_send.at[target],
            recv_sem=back_recv.at[sort, c],
            device_id={"gz": a * GROUP + target},
            device_id_type=MESH,
        )

    def back_arrival(sort, side):
        return pltpu.make_async_remote_copy(
            src_ref=field.at[last, pl.ds(HALO, thin), inner],
            dst_ref=outs[sort].at[:, pl.ds(side * height, height), :],
            send_sem=back_send.at[0],
            recv_sem=back_recv.at[sort, side],
            device_id={"gz": a * GROUP + 2 * sort + side},
            device_id_type=MESH,
        )

    def back_local(sort, target):
        source, landed = back_refs(sort, target)
        return pltpu.make_async_copy(source, landed, back_own.at[0])

    def each_back(remote, own):
        for sort in range(2):
            for target in range(GROUP):

                @pl.when(jnp.logical_and(kind == sort, b != target))
                def _():
                    remote(sort, target)

                if target // 2 == sort:

                    @pl.when(b == target)
                    def _():
                        own(sort, target)

    each_back(
        lambda sort, target: back_remote(sort, target).start(),
        lambda sort, target: back_local(sort, target).start(),
    )
    for sender in range(outer):
        wait_strip(0, sender)
    lax.fori_loop(0, strips.shape[2] // some, first_products, 0)

    def leaving(slab, turn):
        z = pl.ds(slab * layers, layers)
        return (
            pltpu.make_async_copy(light.at[z], light_out.at[z], out_own.at[0, turn]),
            pltpu.make_async_copy(
                raw.at[:, z], raw_out.at[:, z], out_own.at[1, turn]
            ),
        )

    def arrivals(turn, carried):
        slab = (a + turn) % outer
        wait_strip(1, slab)
        last_products(slab)
        for leave in leaving(slab, turn):
            leave.start()
        return carried

    lax.fori_loop(0, outer, arrivals, 0)
    for epoch in range(EPOCHS):
        for target in range(2):

            @pl.when(b != target)
            def _():
                edge_remote(epoch, target, b).wait_send()

    each_back(
        lambda sort, target: back_remote(sort, target).wait_send(),
        lambda sort, target: back_local(sort, target).wait(),
    )
    for sort in range(2):
        for side in range(2):

            @pl.when(b != 2 * sort + side)
            def _():
                back_arrival(sort, side).wait_recv()

    for window in range(SNAPS):
        sent_strips(window)

    def left(turn, carried):
        for leave in leaving((a + turn) % outer, turn):
            leave.wait()
        return carried

    lax.fori_loop(0, outer, left, 0)


def image_kernel(
    raw_in,
    light_in,
    src_in,
    rec_in,
    image_out,
    src_out,
    rec_out,
    raw,
    light,
    finals,
    image,
    inverse,
    light_own,
    raw_own,
    final_own,
    image_own,
):
    lags, depth = raw.shape[:2]
    unit = raw.shape[2:]
    get_light = pltpu.make_async_copy(light_in, light, light_own.at[0])
    get_light.start()
    gets = [
        pltpu.make_async_copy(source, finals.at[index], final_own.at[0, index])
        for index, source in enumerate((src_in, rec_in))
    ]
    puts = [
        pltpu.make_async_copy(finals.at[index], landed, final_own.at[1, index])
        for index, landed in enumerate((src_out, rec_out))
    ]

    def get_raw(index):
        return pltpu.make_async_copy(raw_in.at[index], raw.at[index], raw_own.at[index])

    def put_image(index):
        return pltpu.make_async_copy(
            image.at[index], image_out.at[index], image_own.at[index]
        )

    for get in gets:
        get.start()
    for index in range(lags):
        get_raw(index).start()

    pivots = []
    pivot = 0.0
    for _ in range(depth):
        pivot = 1.0 / (1.0 + 2.0 * smoothing - smoothing * smoothing * pivot)
        pivots.append(float(np.float32(pivot)))
    settled = min(z for z in range(depth) if pivots[z] == pivots[-1])
    settled = min(depth, -(-settled // 8) * 8)
    get_light.wait()

    def forward(z, pivot, carried):
        value = light[z] * pivot + (smoothing * pivot) * carried
        inverse[z] = value
        return value

    def backward(z, pivot, carried):
        value = inverse[z] + (smoothing * pivot) * carried
        inverse[z] = 1.0 / (value + damping)
        return value

    rest = (depth - settled) // 8
    value = jnp.zeros(unit, jnp.float32)
    for z in range(settled):
        value = forward(z, pivots[z], value)

    def down(turn, carried):
        for step in range(8):
            carried = forward(settled + turn * 8 + step, pivots[-1], carried)
        return carried

    lax.fori_loop(0, rest, down, value)
    for get, put in zip(gets, puts):
        get.wait()
        put.start()

    def up(turn, carried):
        for step in range(8):
            carried = backward(depth - 1 - turn * 8 - step, pivots[-1], carried)
        return carried

    value = lax.fori_loop(0, rest, up, jnp.zeros(unit, jnp.float32))
    for z in reversed(range(settled)):
        value = backward(z, pivots[z], value)

    some = 32
    for index in range(lags):
        get_raw(index).wait()

        def layers(block, carried):
            z = pl.ds(block * some, some)
            image[index, z] = (raw[index, z] * inverse[z]).astype(jnp.bfloat16)
            return carried

        lax.fori_loop(0, depth // some, layers, 0)
        put_image(index).start()
    for index in range(lags):
        put_image(index).wait()
    for put in puts:
        put.wait()


def local(
    count,
    shots,
    source_now,
    source_before,
    receiver_now,
    receiver_before,
    speed_term,
    saved_faces,
    face_steps,
    traces,
    lag_offsets,
    snap_phase,
):
    thin, wide, breadth = source_now.shape
    layers = thin * GROUP
    outer = count // GROUP
    half = count // 2
    depth = thin * count
    height = wide // 2
    strip = wide // count
    tall = height * 8 * EPOCH // breadth
    lags = lag_offsets.shape[0]
    me = lax.axis_index("gz")

    hbm = pl.BlockSpec(memory_space=pltpu.HBM)
    smem = pl.BlockSpec(memory_space=pltpu.SMEM)
    dma = pltpu.SemaphoreType.DMA
    flat = jax.ShapeDtypeStruct(source_now.shape, jnp.float32)
    raw, light, source_final, receiver_final = pl.pallas_call(
        functools.partial(wave_kernel, count, shots, strip),
        out_shape=(
            jax.ShapeDtypeStruct((lags, depth, ROWS, breadth), jnp.float32),
            jax.ShapeDtypeStruct((depth, ROWS, breadth), jnp.float32),
            flat,
            flat,
        ),
        in_specs=[smem] + [hbm] * 9,
        out_specs=(hbm, hbm, hbm, hbm),
        scratch_shapes=[
            pltpu.SMEM(snap_phase.shape, jnp.int32),
            pltpu.SMEM(face_steps.shape, jnp.int32),
            pltpu.VMEM(saved_faces.shape, jnp.float32),
            pltpu.VMEM(traces.shape, traces.dtype),
            pltpu.VMEM((2 * breadth, breadth), jnp.bfloat16),
            pltpu.VMEM((breadth, breadth), jnp.bfloat16),
            pltpu.VMEM((2, layers + 2 * HALO, height + 2 * ROWS, breadth), jnp.float32),
            pltpu.VMEM((layers, height, breadth), jnp.float32),
            pltpu.VMEM((EPOCHS, 2, thin, tall, breadth), jnp.float32),
            pltpu.VMEM((EPOCHS, layers, tall, breadth), jnp.float32),
            pltpu.VMEM((2, 2, HALO, height, breadth), jnp.float32),
            pltpu.VMEM((SNAPS, layers, height, breadth), jnp.float32),
            pltpu.VMEM((SNAPS, 2, depth, ROWS, breadth), jnp.float32),
            pltpu.VMEM((lags, depth, ROWS, breadth), jnp.float32),
            pltpu.VMEM((depth, ROWS, breadth), jnp.float32),
            dma((4,)),
            dma((3, GROUP)),
            dma((3, GROUP)),
            dma((3,)),
            dma((2,)),
            dma((2,)),
            dma((EPOCHS, 2)),
            dma((EPOCHS, GROUP)),
            dma((2, 2, PIECES)),
            dma((2, 2, PIECES)),
            dma((2,)),
            dma((2,)),
            dma((SNAPS, half)),
            dma((SNAPS, 2, outer)),
            dma((SNAPS,)),
            dma((GROUP,)),
            dma((2, 2)),
            dma((1,)),
            dma((2, outer)),
        ],
        compiler_params=pltpu.CompilerParams(
            has_side_effects=True,
            vmem_limit_bytes=VMEM_BYTES,
            collective_id=0 if close_barrier(outer) else None,
        ),
        name="waves",
    )(
        lag_offsets,
        snap_phase,
        face_steps,
        source_now,
        source_before,
        receiver_now,
        receiver_before,
        speed_term,
        saved_faces,
        traces,
    )

    if strip < ROWS:
        place = (me * strip) % ROWS
        raw = lax.dynamic_slice_in_dim(raw, place, strip, 2)
        light = lax.dynamic_slice_in_dim(light, place, strip, 1)
    image_shape = (lags, depth, strip, breadth)
    return pl.pallas_call(
        image_kernel,
        out_shape=(jax.ShapeDtypeStruct(image_shape, jnp.bfloat16), flat, flat),
        in_specs=[hbm] * 4,
        out_specs=(hbm, hbm, hbm),
        scratch_shapes=[
            pltpu.VMEM(raw.shape, jnp.float32),
            pltpu.VMEM(light.shape, jnp.float32),
            pltpu.VMEM((2,) + source_now.shape, jnp.float32),
            pltpu.VMEM(image_shape, jnp.bfloat16),
            pltpu.VMEM(light.shape, jnp.float32),
            dma((1,)),
            dma((lags,)),
            dma((2, 2)),
            dma((lags,)),
        ],
        compiler_params=pltpu.CompilerParams(vmem_limit_bytes=VMEM_BYTES),
        name="images",
    )(raw, light, source_final, receiver_final)


def solution(mesh):
    return jax.shard_map(
        functools.partial(local, mesh.shape["gz"], mesh.shape["shot"]),
        mesh=mesh,
        in_specs=(
            P(("shot", "gz"), None, None),
            P(("shot", "gz"), None, None),
            P(("shot", "gz"), None, None),
            P(("shot", "gz"), None, None),
            P("gz", None, None),
            P("shot", None, "gz", None),
            P(),
            P("shot", None, None),
            P(),
            P(),
        ),
        out_specs=(
            P("shot", None, "gz", None),
            P(("shot", "gz"), None, None),
            P(("shot", "gz"), None, None),
        ),
        check_vma=False,
    )
```

```python
import functools

import jax
import jax.numpy as jnp
import numpy as np
from jax import lax
from jax.experimental import pallas as pl
from jax.experimental.pallas import tpu as pltpu
from jax.sharding import PartitionSpec as P

SNAP_EVERY = 6
SNAPS = 2
STEPS = SNAPS * SNAP_EVERY
HALO = 4
ROWS = 8
CHUNK = 4
GROUP = 4
PIECES = 8
EPOCH = 4
VMEM_BYTES = 60 * 1024 * 1024
EPOCHS = STEPS // EPOCH

stencil_weights = (-205.0 / 72.0, 8.0 / 5.0, -1.0 / 5.0, 8.0 / 315.0, -1.0 / 560.0)
damping = 0.25
smoothing = 16.0
MESH = pl.DeviceIdType.MESH


def lateral_weights(breadth):
    apart = jnp.abs(
        lax.broadcasted_iota(jnp.int32, (breadth, breadth), 0)
        - lax.broadcasted_iota(jnp.int32, (breadth, breadth), 1)
    )
    band = jnp.where(apart == 0, 3.0 * stencil_weights[0], 0.0)
    for offset in range(1, 5):
        band = jnp.where(apart == offset, stencil_weights[offset], band)
    high = band.astype(jnp.bfloat16)
    low = (band - high.astype(jnp.float32)).astype(jnp.bfloat16)
    return high, low


def close_barrier(outer):
    return outer <= SNAP_EVERY


def wave_kernel(
    count,
    shots,
    strip,
    lag_ref,
    phase_hbm,
    order_hbm,
    src_now,
    src_old,
    rec_now,
    rec_old,
    speed,
    faces_hbm,
    traces_hbm,
    raw_out,
    light_out,
    src_out,
    rec_out,
    phase_ref,
    order_ref,
    faces,
    traces,
    weights_a,
    weights_b,
    field,
    factor,
    packed,
    edges,
    halo,
    snaps,
    strips,
    raw,
    light,
    small_own,
    load_send,
    load_recv,
    load_own,
    relay_send,
    relay_recv,
    edge_send,
    edge_recv,
    z_send,
    z_recv,
    row_send,
    row_recv,
    strip_send,
    strip_recv,
    strip_own,
    back_send,
    back_recv,
    back_own,
    out_own,
):
    me = lax.axis_index("gz")
    outer = count // GROUP
    a = me // GROUP
    b = me % GROUP
    kind = b // 2
    c = b % 2
    thin = src_now.shape[0]
    layers = thin * GROUP
    height = src_now.shape[1] // 2
    breadth = src_now.shape[2]
    inner = pl.ds(ROWS, height)
    now_of = (src_now, rec_now)
    old_of = (src_old, rec_old)
    outs = (src_out, rec_out)

    paired = shots % 2 == 0
    shot = lax.axis_index("shot")
    parity = shot % 2
    other_shot = {"shot": shot + 1 - 2 * parity, "gz": me}

    if close_barrier(outer):
        barrier = pltpu.get_barrier_semaphore()

        def greet(device):
            pl.semaphore_signal(barrier, inc=1, device_id=device, device_id_type=MESH)

        for shift in range(1, GROUP):
            greet({"gz": a * GROUP + (b + shift) % GROUP})
        if paired:
            greet(other_shot)

        @pl.when(a > 0)
        def _():
            greet({"gz": me - GROUP})

        @pl.when(a < outer - 1)
        def _():
            greet({"gz": me + GROUP})

        beside = (a > 0, a < outer - 1)
        for count_beside, met in (
            (2, jnp.logical_and(*beside)),
            (1, beside[0] != beside[1]),
            (0, jnp.logical_not(jnp.logical_or(*beside))),
        ):

            @pl.when(met)
            def _():
                pl.semaphore_wait(barrier, GROUP - 1 + paired + count_beside)

    def load_refs(index, target, sender):
        rows = pl.ds(target % 2 * height, height)
        planes = pl.ds(HALO + sender * thin, thin)
        source = (speed, now_of[target // 2], old_of[target // 2])[index]
        landed = (
            factor.at[pl.ds(sender * thin, thin)],
            field.at[0, planes, inner],
            field.at[1, planes, inner],
        )[index]
        return source.at[:, rows, :], landed

    def load_remote(index, target, sender):
        source, landed = load_refs(index, target, sender)
        return pltpu.make_async_remote_copy(
            src_ref=source,
            dst_ref=landed,
            send_sem=load_send.at[index, target],
            recv_sem=load_recv.at[index, sender],
            device_id={"gz": a * GROUP + target},
            device_id_type=MESH,
        )

    def load_local(index, target):
        source, landed = load_refs(index, target, target)
        return pltpu.make_async_copy(source, landed, load_own.at[index])

    def direct(index, target):
        if index > 0 or not paired:
            return b != target
        near = jnp.logical_or(kind == target // 2, parity == target % 2)
        return jnp.logical_and(b != target, near)

    def relay(sender):
        view = factor.at[pl.ds(sender * thin, thin)]
        return pltpu.make_async_remote_copy(
            src_ref=view,
            dst_ref=view,
            send_sem=relay_send.at[sender % 2],
            recv_sem=relay_recv.at[sender % 2],
            device_id=other_shot,
            device_id_type=MESH,
        )

    small = (
        (faces_hbm, faces),
        (order_hbm, order_ref),
        (phase_hbm, phase_ref),
        (traces_hbm, traces),
    )

    def fetch(index):
        source, landed = small[index]
        return pltpu.make_async_copy(source, landed, small_own.at[index])

    for index in range(3):
        for target in range(GROUP):

            @pl.when(direct(index, target))
            def _():
                load_remote(index, target, b).start()

    for index in range(len(small)):
        fetch(index).start()
    for index in range(3):
        for target in range(GROUP):

            @pl.when(b == target)
            def _():
                load_local(index, target).start()

    def wait_load(index):
        for sender in range(GROUP):

            @pl.when(b == sender)
            def _():
                load_local(index, sender).wait()

            if index > 0 or not paired:

                @pl.when(b != sender)
                def _():
                    load_remote(index, sender, sender).wait_recv()

            else:

                @pl.when(jnp.logical_and(b != sender, kind == sender // 2))
                def _():
                    load_remote(index, sender, sender).wait_recv()

                @pl.when(jnp.logical_and(kind != sender // 2, parity != c))
                def _():
                    relay(sender).wait_recv()

    def pass_on():
        for sender in range(GROUP):

            @pl.when(jnp.logical_and(kind != sender // 2, parity == c))
            def _():
                load_remote(0, sender, sender).wait_recv()
                relay(sender).start()

    def passed_on():
        for sender in range(GROUP):

            @pl.when(jnp.logical_and(kind != sender // 2, parity == c))
            def _():
                relay(sender).wait_send()

    high, low = lateral_weights(breadth)
    weights_a[pl.ds(0, breadth)] = high
    weights_a[pl.ds(breadth, breadth)] = high
    weights_b[...] = low
    fetch(0).wait()
    fetch(1).wait()

    lane = lax.broadcasted_iota(jnp.int32, (1, 1, breadth), 2)
    across = 8 * EPOCH
    groups = breadth // across
    tall = height // groups
    tiles_a_part = tall // ROWS
    for z in range(thin):
        parts = [
            pltpu.roll(faces[order_ref[step], :, z, :], 4, 0) for step in range(STEPS)
        ]
        parts.append(jnp.zeros((breadth - 8 * STEPS, 2 * height), jnp.float32))
        turned = jnp.concatenate(parts, axis=0).T
        for epoch in range(EPOCHS):
            for half in range(2):
                block = None
                for part in range(groups):
                    first = half * height + part * tall
                    moved = turned[first : first + tall]
                    turn = (across * (part - epoch)) % breadth
                    if turn:
                        moved = pltpu.roll(moved, turn, 1)
                    if block is None:
                        block = moved
                    else:
                        block = jnp.where(lane[0] >= across * part, moved, block)
                packed[epoch, half, z] = block

    def edge_remote(epoch, target, sender):
        return pltpu.make_async_remote_copy(
            src_ref=packed.at[epoch, target],
            dst_ref=edges.at[epoch, pl.ds(sender * thin, thin)],
            send_sem=edge_send.at[epoch, target],
            recv_sem=edge_recv.at[epoch, sender],
            device_id={"gz": a * GROUP + target},
            device_id_type=MESH,
        )

    for epoch in range(EPOCHS):
        for target in range(2):

            @pl.when(b != target)
            def _():
                edge_remote(epoch, target, b).start()

            @pl.when(b == target)
            def _():
                edges[epoch, pl.ds(target * thin, thin)] = packed[epoch, target]

    def wait_edge(epoch):
        for sender in range(GROUP):

            @pl.when(jnp.logical_and(kind == 0, b != sender))
            def _():
                edge_remote(epoch, 0, sender).wait_recv()

    for slot in range(2):
        for first in (0, HALO + layers):
            field[slot, pl.ds(first, HALO), inner] = jnp.zeros(
                (HALO, height, breadth), jnp.float32
            )

        @pl.when(c == 0)
        def _():
            field[slot, pl.ds(HALO, layers), pl.ds(0, ROWS)] = jnp.zeros(
                (layers, ROWS, breadth), jnp.float32
            )

        @pl.when(c == 1)
        def _():
            field[slot, pl.ds(HALO, layers), pl.ds(ROWS + height, ROWS)] = jnp.zeros(
                (layers, ROWS, breadth), jnp.float32
            )

        @pl.when(a == 0)
        def _():
            halo[0, slot] = jnp.zeros((HALO, height, breadth), jnp.float32)

        @pl.when(a == outer - 1)
        def _():
            halo[1, slot] = jnp.zeros((HALO, height, breadth), jnp.float32)

    snaps[...] = jnp.zeros(snaps.shape, jnp.float32)

    span = height // PIECES
    present = (a > 0, a < outer - 1)

    def z_copy(side, piece, slot):
        return pltpu.make_async_remote_copy(
            src_ref=field.at[
                slot,
                pl.ds((HALO, layers)[side], HALO),
                pl.ds(ROWS + piece * span, span),
            ],
            dst_ref=halo.at[1 - side, slot, :, pl.ds(piece * span, span)],
            send_sem=z_send.at[side, slot, piece],
            recv_sem=z_recv.at[1 - side, slot, piece],
            device_id={"gz": (me - GROUP, me + GROUP)[side]},
            device_id_type=MESH,
        )

    def send_z(piece, slot, also=None):
        for side in range(2):
            allowed = present[side]
            if also is not None:
                allowed = jnp.logical_and(allowed, also)

            @pl.when(allowed)
            def _():
                z_copy(side, piece, slot).start()

    def wait_z(piece, slot):
        for side in range(2):

            @pl.when(present[side])
            def _():
                z_copy(1 - side, piece, slot).wait_recv()

    def sent_z(slot):
        for side in range(2):

            @pl.when(present[side])
            def _():
                for piece in range(PIECES):
                    z_copy(side, piece, slot).wait_send()

    body = pl.ds(HALO, layers)

    def row_copy(way, slot):
        first, landed = (
            (ROWS + height - HALO, ROWS - HALO),
            (ROWS, ROWS + height),
        )[way]
        return pltpu.make_async_remote_copy(
            src_ref=field.at[slot, body, pl.ds(first, HALO)],
            dst_ref=field.at[slot, body, pl.ds(landed, HALO)],
            send_sem=row_send.at[slot],
            recv_sem=row_recv.at[slot],
            device_id={"gz": me + 1 - 2 * c},
            device_id_type=MESH,
        )

    def each_way(do, also=None):
        for way in range(2):
            allowed = c == way
            if also is not None:
                allowed = jnp.logical_and(allowed, also)

            @pl.when(allowed)
            def _():
                do(way)

    def send_row(slot, also=None):
        each_way(lambda way: row_copy(way, slot).start(), also)

    def wait_row(slot):
        each_way(lambda way: row_copy(1 - way, slot).wait_recv())

    def sent_row(slot):
        each_way(lambda way: row_copy(way, slot).wait_send())

    outside = ((lane < 4) | (lane >= breadth - 4)) & (kind == 0)
    lit = jnp.logical_and(a == 0, kind == 1)

    tiles = height // ROWS

    def partial(step, now, later, base, deep, first, many, top=False):
        planes = pl.ds(HALO + base, deep)
        start = first * ROWS
        if not isinstance(first, int):
            start = pl.multiple_of(start, ROWS)
        tall = many * ROWS
        rows = pl.ds(ROWS + start, tall)
        window = field[now, planes, pl.ds(start, tall + 2 * ROWS), :]
        center = window[:, ROWS : ROWS + tall]
        flat = center.reshape(deep * tall, breadth)
        high = flat.astype(jnp.bfloat16)
        low = (flat - high.astype(jnp.float32)).astype(jnp.bfloat16)
        lateral = jnp.dot(
            jnp.concatenate([high, low], axis=1),
            weights_a[...],
            preferred_element_type=jnp.float32,
        ) + jnp.dot(high, weights_b[...], preferred_element_type=jnp.float32)
        summed = lateral.reshape(deep, tall, breadth)
        for offset in range(1, 5):
            summed = summed + stencil_weights[offset] * (
                (
                    field[now, pl.ds(HALO + base + offset, deep), rows, :]
                    + field[now, pl.ds(HALO + base - offset, deep), rows, :]
                )
                + (
                    window[:, ROWS + offset : ROWS + offset + tall]
                    + window[:, ROWS - offset : ROWS - offset + tall]
                )
            )
        previous = field[later, planes, rows, :]
        speeds = factor[pl.ds(base, deep), pl.ds(start, tall)]
        updated = 2.0 * center - previous + speeds * summed
        placed = []
        for tile in range(many):
            place = first + tile
            inside = place % tiles_a_part * ROWS
            if not isinstance(place, int):
                inside = pl.multiple_of(inside, ROWS)
            edge = edges[step // EPOCH, pl.ds(base, deep), pl.ds(inside, ROWS)]
            turn = 3 * breadth - 4 - across * (place // tiles_a_part)
            turn = lax.rem(turn - 8 * (step % EPOCH), breadth)
            edge = pltpu.roll(edge.reshape(deep * ROWS, breadth), turn, 1)
            placed.append(edge.reshape(deep, ROWS, breadth))
        placed = placed[0] if many == 1 else jnp.concatenate(placed, axis=1)
        updated = jnp.where(outside, placed, updated)
        if top:
            trace = traces[step, pl.ds(pl.multiple_of(c * height, height), height)]
            trace = jnp.where(lit, trace.astype(jnp.float32), 0.0)
            updated = jnp.concatenate([updated[:1] + trace[None], updated[1:]], axis=0)
        return updated

    def keep(window, take, base, rows, value):
        held = snaps[window, pl.ds(base, value.shape[0]), rows]
        snaps[window, pl.ds(base, value.shape[0]), rows] = jnp.where(take, value, held)

    def complete(window, take, now, later, piece):
        rows = pl.ds(piece * span, span)
        wide = pl.ds(ROWS + piece * span, span)
        for side in range(2):
            base = (0, layers - HALO)[side]
            held = [halo[side, now, near, rows] for near in range(HALO)]
            added = []
            for near in range(HALO):
                total = None
                reach = HALO - near if side == 0 else near + 1
                for k in range(reach):
                    offset = HALO - k
                    index = near + k if side == 0 else near - k
                    term = stencil_weights[offset] * held[index]
                    total = term if total is None else total + term
                added.append(total[None])
            added = jnp.concatenate(added, axis=0)
            planes = pl.ds(HALO + base, HALO)
            added = jnp.where(outside, 0.0, factor[pl.ds(base, HALO), rows] * added)
            value = field[later, planes, wide] + added
            field[later, planes, wide] = value
            keep(window, take, base, rows, value)

    def whole_step(window, local):
        step = window * SNAP_EVERY + local
        now = lax.rem(step, 2)
        later = 1 - now
        more = step < STEPS - 1
        take = phase_ref[window] == local

        @pl.when(lax.rem(step, EPOCH) == 0)
        def _():
            wait_edge(step // EPOCH)

        wait_row(now)
        for base, top in ((0, True), (layers - HALO, False)):
            field[later, pl.ds(HALO + base, HALO), inner] = partial(
                step, now, later, base, HALO, 0, tiles, top
            )
        for piece in range(PIECES):
            wait_z(piece, now)
            complete(window, take, now, later, piece)
            send_z(piece, later, more)

        def interior(base, deep, first, many):
            start = pl.multiple_of(first * ROWS, ROWS)
            value = partial(step, now, later, base, deep, first, many)
            rows = pl.ds(ROWS + start, many * ROWS)
            field[later, pl.ds(HALO + base, deep), rows] = value
            keep(window, take, base, pl.ds(start, many * ROWS), value)

        interior(HALO, layers - 2 * HALO, (1 - c) * (tiles - 1), 1)
        send_row(later, more)

        def middle(chunk, carried):
            interior(chunk * CHUNK, CHUNK, c, tiles - 1)
            return carried

        lax.fori_loop(1, layers // CHUNK - 1, middle, 0)
        sent_z(now)
        sent_row(now)

    half = count // 2

    def strip_refs(window, index):
        first = pl.multiple_of(index * strip // ROWS * ROWS, ROWS)
        return (
            snaps.at[window, :, pl.ds(first, ROWS), :],
            strips.at[window, kind, pl.ds(a * layers, layers)],
        )

    def strip_remote(window, index, sender, sort):
        source = snaps.at[
            window, :, pl.ds(pl.multiple_of(index * strip // ROWS * ROWS, ROWS), ROWS), :
        ]
        return pltpu.make_async_remote_copy(
            src_ref=source,
            dst_ref=strips.at[window, sort, pl.ds(sender * layers, layers)],
            send_sem=strip_send.at[window, index],
            recv_sem=strip_recv.at[window, sort, sender],
            device_id={"gz": c * half + index},
            device_id_type=MESH,
        )

    def strip_local(window, index):
        source, landed = strip_refs(window, index)
        return pltpu.make_async_copy(source, landed, strip_own.at[window])

    def start_strip(window, turn):
        index = (turn + GROUP * a + 2 * kind) % half
        target = c * half + index

        @pl.when(jnp.logical_and(target != me, turn < half))
        def _():
            strip_remote(window, index, a, kind).start()

        @pl.when(jnp.logical_and(target == me, turn < half))
        def _():
            strip_local(window, index).start()

    def sent_strips(window):
        def sent(index, carried):
            target = c * half + index

            @pl.when(target != me)
            def _():
                strip_remote(window, index, a, kind).wait_send()

            return carried

        lax.fori_loop(0, half, sent, 0)

    def wait_strip(window, sender):
        for sort in range(2):
            source = sender * GROUP + 2 * sort + me // half

            @pl.when(source != me)
            def _():
                strip_remote(window, 0, sender, sort).wait_recv()

            @pl.when(source == me)
            def _():
                strip_local(window, me % half).wait()

    lags = raw.shape[0]
    some = 16
    unit = (ROWS, breadth)
    column = lax.broadcasted_iota(jnp.int32, unit, 1)

    def first_products(block, carried):
        z = pl.ds(block * some, some)
        shot_wave = strips[0, 0, z]
        echo = strips[0, 1, z]
        light[z] = shot_wave * shot_wave
        for index in range(lags):
            back = lax.rem(2 * breadth - 2 * lag_ref[index], breadth)
            raw[index, z] = shot_wave * pltpu.roll(echo, back, 2)
        return carried

    def last_products(slab):
        def block_products(block, carried):
            z = pl.ds(slab * layers + block * some, some)
            shot_wave = strips[1, 0, z]
            echo = strips[1, 1, z]
            light[z] = light[z] + shot_wave * shot_wave
            for index in range(lags):
                lag = lag_ref[index]
                reach = jnp.abs(lag)
                inside = (column >= reach) & (column < breadth - reach)
                back = lax.rem(2 * breadth - 2 * lag, breadth)
                forth = lax.rem(breadth + lag, breadth)
                total = raw[index, z] + shot_wave * pltpu.roll(echo, back, 2)
                raw[index, z] = jnp.where(
                    inside[None], pltpu.roll(total, forth, 2), 0.0
                )
            return carried

        lax.fori_loop(0, layers // some, block_products, 0)

    if paired:
        pass_on()
    wait_load(1)
    for piece in range(PIECES):
        send_z(piece, 0)
    send_row(0)
    wait_load(0)
    wait_load(2)
    fetch(2).wait()
    fetch(3).wait()
    for index in range(3):
        for target in range(GROUP):

            @pl.when(direct(index, target))
            def _():
                load_remote(index, target, b).wait_send()

    if paired:
        passed_on()

    share = (half + SNAP_EVERY - 1) // SNAP_EVERY
    for window in range(SNAPS):

        def both(local, carried):
            whole_step(window, local)
            if window > 0:
                for part in range(share):
                    start_strip(window - 1, local * share + part)
            return carried

        lax.fori_loop(0, SNAP_EVERY, both, 0)
    lax.fori_loop(0, half, lambda turn, carried: (start_strip(SNAPS - 1, turn), carried)[1], 0)

    last = STEPS % 2

    def back_refs(sort, target):
        return (
            field.at[last, pl.ds(HALO + target * thin, thin), inner],
            outs[sort].at[:, pl.ds(pl.multiple_of(c * height, height), height), :],
        )

    def back_remote(sort, target):
        source, landed = back_refs(sort, target)
        return pltpu.make_async_remote_copy(
            src_ref=source,
            dst_ref=landed,
            send_sem=back_send.at[target],
            recv_sem=back_recv.at[sort, c],
            device_id={"gz": a * GROUP + target},
            device_id_type=MESH,
        )

    def back_arrival(sort, side):
        return pltpu.make_async_remote_copy(
            src_ref=field.at[last, pl.ds(HALO, thin), inner],
            dst_ref=outs[sort].at[:, pl.ds(side * height, height), :],
            send_sem=back_send.at[0],
            recv_sem=back_recv.at[sort, side],
            device_id={"gz": a * GROUP + 2 * sort + side},
            device_id_type=MESH,
        )

    def back_local(sort, target):
        source, landed = back_refs(sort, target)
        return pltpu.make_async_copy(source, landed, back_own.at[0])

    def each_back(remote, own):
        for sort in range(2):
            for target in range(GROUP):

                @pl.when(jnp.logical_and(kind == sort, b != target))
                def _():
                    remote(sort, target)

                if target // 2 == sort:

                    @pl.when(b == target)
                    def _():
                        own(sort, target)

    each_back(
        lambda sort, target: back_remote(sort, target).start(),
        lambda sort, target: back_local(sort, target).start(),
    )
    for sender in range(outer):
        wait_strip(0, sender)
    lax.fori_loop(0, strips.shape[2] // some, first_products, 0)

    def leaving(slab, turn):
        z = pl.ds(slab * layers, layers)
        return (
            pltpu.make_async_copy(light.at[z], light_out.at[z], out_own.at[0, turn]),
            pltpu.make_async_copy(
                raw.at[:, z], raw_out.at[:, z], out_own.at[1, turn]
            ),
        )

    def arrivals(turn, carried):
        slab = (a + turn) % outer
        wait_strip(1, slab)
        last_products(slab)
        for leave in leaving(slab, turn):
            leave.start()
        return carried

    lax.fori_loop(0, outer, arrivals, 0)
    for epoch in range(EPOCHS):
        for target in range(2):

            @pl.when(b != target)
            def _():
                edge_remote(epoch, target, b).wait_send()

    each_back(
        lambda sort, target: back_remote(sort, target).wait_send(),
        lambda sort, target: back_local(sort, target).wait(),
    )
    for sort in range(2):
        for side in range(2):

            @pl.when(b != 2 * sort + side)
            def _():
                back_arrival(sort, side).wait_recv()

    for window in range(SNAPS):
        sent_strips(window)

    def left(turn, carried):
        for leave in leaving((a + turn) % outer, turn):
            leave.wait()
        return carried

    lax.fori_loop(0, outer, left, 0)


def image_kernel(
    raw_in,
    light_in,
    src_in,
    rec_in,
    image_out,
    src_out,
    rec_out,
    raw,
    light,
    finals,
    image,
    inverse,
    light_own,
    raw_own,
    final_own,
    image_own,
):
    lags, depth = raw.shape[:2]
    unit = raw.shape[2:]
    get_light = pltpu.make_async_copy(light_in, light, light_own.at[0])
    get_light.start()
    gets = [
        pltpu.make_async_copy(source, finals.at[index], final_own.at[0, index])
        for index, source in enumerate((src_in, rec_in))
    ]
    puts = [
        pltpu.make_async_copy(finals.at[index], landed, final_own.at[1, index])
        for index, landed in enumerate((src_out, rec_out))
    ]

    def get_raw(index):
        return pltpu.make_async_copy(raw_in.at[index], raw.at[index], raw_own.at[index])

    def put_image(index):
        return pltpu.make_async_copy(
            image.at[index], image_out.at[index], image_own.at[index]
        )

    for get in gets:
        get.start()
    for index in range(lags):
        get_raw(index).start()

    pivots = []
    pivot = 0.0
    for _ in range(depth):
        pivot = 1.0 / (1.0 + 2.0 * smoothing - smoothing * smoothing * pivot)
        pivots.append(float(np.float32(pivot)))
    settled = min(z for z in range(depth) if pivots[z] == pivots[-1])
    settled = min(depth, -(-settled // 8) * 8)
    get_light.wait()

    def forward(z, pivot, carried):
        value = light[z] * pivot + (smoothing * pivot) * carried
        inverse[z] = value
        return value

    def backward(z, pivot, carried):
        value = inverse[z] + (smoothing * pivot) * carried
        inverse[z] = 1.0 / (value + damping)
        return value

    rest = (depth - settled) // 8
    value = jnp.zeros(unit, jnp.float32)
    for z in range(settled):
        value = forward(z, pivots[z], value)

    def down(turn, carried):
        for step in range(8):
            carried = forward(settled + turn * 8 + step, pivots[-1], carried)
        return carried

    lax.fori_loop(0, rest, down, value)
    for get, put in zip(gets, puts):
        get.wait()
        put.start()

    def up(turn, carried):
        for step in range(8):
            carried = backward(depth - 1 - turn * 8 - step, pivots[-1], carried)
        return carried

    value = lax.fori_loop(0, rest, up, jnp.zeros(unit, jnp.float32))
    for z in reversed(range(settled)):
        value = backward(z, pivots[z], value)

    some = 32
    for index in range(lags):
        get_raw(index).wait()

        def layers(block, carried):
            z = pl.ds(block * some, some)
            image[index, z] = (raw[index, z] * inverse[z]).astype(jnp.bfloat16)
            return carried

        lax.fori_loop(0, depth // some, layers, 0)
        put_image(index).start()
    for index in range(lags):
        put_image(index).wait()
    for put in puts:
        put.wait()


def local(
    count,
    shots,
    source_now,
    source_before,
    receiver_now,
    receiver_before,
    speed_term,
    saved_faces,
    face_steps,
    traces,
    lag_offsets,
    snap_phase,
):
    thin, wide, breadth = source_now.shape
    layers = thin * GROUP
    outer = count // GROUP
    half = count // 2
    depth = thin * count
    height = wide // 2
    strip = wide // count
    tall = height * 8 * EPOCH // breadth
    lags = lag_offsets.shape[0]
    me = lax.axis_index("gz")

    hbm = pl.BlockSpec(memory_space=pltpu.HBM)
    smem = pl.BlockSpec(memory_space=pltpu.SMEM)
    dma = pltpu.SemaphoreType.DMA
    flat = jax.ShapeDtypeStruct(source_now.shape, jnp.float32)
    raw, light, source_final, receiver_final = pl.pallas_call(
        functools.partial(wave_kernel, count, shots, strip),
        out_shape=(
            jax.ShapeDtypeStruct((lags, depth, ROWS, breadth), jnp.float32),
            jax.ShapeDtypeStruct((depth, ROWS, breadth), jnp.float32),
            flat,
            flat,
        ),
        in_specs=[smem] + [hbm] * 9,
        out_specs=(hbm, hbm, hbm, hbm),
        scratch_shapes=[
            pltpu.SMEM(snap_phase.shape, jnp.int32),
            pltpu.SMEM(face_steps.shape, jnp.int32),
            pltpu.VMEM(saved_faces.shape, jnp.float32),
            pltpu.VMEM(traces.shape, traces.dtype),
            pltpu.VMEM((2 * breadth, breadth), jnp.bfloat16),
            pltpu.VMEM((breadth, breadth), jnp.bfloat16),
            pltpu.VMEM((2, layers + 2 * HALO, height + 2 * ROWS, breadth), jnp.float32),
            pltpu.VMEM((layers, height, breadth), jnp.float32),
            pltpu.VMEM((EPOCHS, 2, thin, tall, breadth), jnp.float32),
            pltpu.VMEM((EPOCHS, layers, tall, breadth), jnp.float32),
            pltpu.VMEM((2, 2, HALO, height, breadth), jnp.float32),
            pltpu.VMEM((SNAPS, layers, height, breadth), jnp.float32),
            pltpu.VMEM((SNAPS, 2, depth, ROWS, breadth), jnp.float32),
            pltpu.VMEM((lags, depth, ROWS, breadth), jnp.float32),
            pltpu.VMEM((depth, ROWS, breadth), jnp.float32),
            dma((4,)),
            dma((3, GROUP)),
            dma((3, GROUP)),
            dma((3,)),
            dma((2,)),
            dma((2,)),
            dma((EPOCHS, 2)),
            dma((EPOCHS, GROUP)),
            dma((2, 2, PIECES)),
            dma((2, 2, PIECES)),
            dma((2,)),
            dma((2,)),
            dma((SNAPS, half)),
            dma((SNAPS, 2, outer)),
            dma((SNAPS,)),
            dma((GROUP,)),
            dma((2, 2)),
            dma((1,)),
            dma((2, outer)),
        ],
        compiler_params=pltpu.CompilerParams(
            has_side_effects=True,
            vmem_limit_bytes=VMEM_BYTES,
            collective_id=0 if close_barrier(outer) else None,
        ),
        name="waves",
    )(
        lag_offsets,
        snap_phase,
        face_steps,
        source_now,
        source_before,
        receiver_now,
        receiver_before,
        speed_term,
        saved_faces,
        traces,
    )

    if strip < ROWS:
        place = (me * strip) % ROWS
        raw = lax.dynamic_slice_in_dim(raw, place, strip, 2)
        light = lax.dynamic_slice_in_dim(light, place, strip, 1)
    image_shape = (lags, depth, strip, breadth)
    return pl.pallas_call(
        image_kernel,
        out_shape=(jax.ShapeDtypeStruct(image_shape, jnp.bfloat16), flat, flat),
        in_specs=[hbm] * 4,
        out_specs=(hbm, hbm, hbm),
        scratch_shapes=[
            pltpu.VMEM(raw.shape, jnp.float32),
            pltpu.VMEM(light.shape, jnp.float32),
            pltpu.VMEM((2,) + source_now.shape, jnp.float32),
            pltpu.VMEM(image_shape, jnp.bfloat16),
            pltpu.VMEM(light.shape, jnp.float32),
            dma((1,)),
            dma((lags,)),
            dma((2, 2)),
            dma((lags,)),
        ],
        compiler_params=pltpu.CompilerParams(vmem_limit_bytes=VMEM_BYTES),
        name="images",
    )(raw, light, source_final, receiver_final)


def solution(mesh):
    return jax.shard_map(
        functools.partial(local, mesh.shape["gz"], mesh.shape["shot"]),
        mesh=mesh,
        in_specs=(
            P(("shot", "gz"), None, None),
            P(("shot", "gz"), None, None),
            P(("shot", "gz"), None, None),
            P(("shot", "gz"), None, None),
            P("gz", None, None),
            P("shot", None, "gz", None),
            P(),
            P("shot", None, None),
            P(),
            P(),
        ),
        out_specs=(
            P("shot", None, "gz", None),
            P(("shot", "gz"), None, None),
            P(("shot", "gz"), None, None),
        ),
        check_vma=False,
    )
```
